256 devices in a mesh: gz: 8 (over z), gx: 4 (over x), gy: 8 (over y, core).
Axes of the slice: x: 4, y: 4, z: 8, core: 2. Of those that a mesh axis runs over, the one named last changes fastest.
Arguments:
- density: float32 [256, 1024, 1024], P('gz', 'gy', 'gx'), may hold values from 0 to 1
- mask: int32 [32, 128, 128], P('gz', 'gy', 'gx'), may hold values from 0 to 3
Outputs:
- filtered: float32 [256, 1024, 1024], P(('gz', 'gx'), 'gy')
- projected: float32 [256, 1024, 1024], P(('gz', 'gx'), 'gy')
The draws below stay inside these ranges and needn't reach their ends.
Inputs may be any that keep to these rules, and one draw needn't show every extreme that they name: `mask`: code 0 marks a void block, 1 a solid block, 2 and 3 design blocks.
All inputs are finite; a program needn't handle non-finite values.
Results may differ from the reference program's by a relative error of at most 0.0003.
Values sent between devices are 32-bit elements; how exact they have to be, the bound alone decides.
A program may use at most 128 MiB of HBM per device.

```python
import jax
import jax.numpy as jnp
from jax import lax

RADIUS = 6
CELLS = 8
NX = 1024
NY = 1024
NZ = 256


def set_ends(drawn, rng, smallest, high):
    dims = drawn.shape
    spot = [jax.random.randint(jax.random.fold_in(rng, axis), (), 0, dims[axis]) for axis in range(len(dims))]
    drawn = drawn.at[tuple(spot)].set(smallest)
    longest = dims.index(max(dims))
    spot[longest] = (spot[longest] + 1) % dims[longest]
    return drawn.at[tuple(spot)].set(high)


def steps_of(stream_key, shape, split, low, high):
    level = 1.0
    for dim, parts in split:
        steps = jax.random.uniform(jax.random.fold_in(jax.random.fold_in(stream_key, 6), dim), (parts,), jnp.float32, low / len(split), high / len(split))
        level = level * jnp.repeat(jnp.exp(steps), shape[dim] // parts).reshape((-1,) + (1,) * (len(shape) - 1 - dim))
    return level


def setup_inputs(seed: int = 0) -> dict:
    splits = jax.random.split(jax.random.key(seed), 3)
    return {
        "density": jnp.clip(1.0 * jax.random.uniform(splits[0], (NZ, NY, NX), jnp.float32) ** steps_of(splits[0], (NZ, NY, NX), ((0, 8), (1, 8), (2, 4)), -0.2, 0.2), 0.0, 1.0),
        "mask": set_ends(jax.random.randint(splits[1], (NZ // CELLS, NY // CELLS, NX // CELLS), 0, 4), jax.random.fold_in(splits[1], 1), 0, 3).astype(jnp.int32),
    }


sharpness = 8.0
threshold = 0.5


def smooth_axis(values, axis_index, count):
    widths = [(RADIUS, RADIUS) if position == axis_index else (0, 0) for position in range(values.ndim)]
    padded = jnp.pad(values, widths)
    result = jnp.zeros_like(values)
    for offset in range(-RADIUS, RADIUS + 1):
        window = lax.slice_in_dim(padded, RADIUS + offset, RADIUS + offset + count, axis=axis_index)
        result = result + float(RADIUS + 1 - abs(offset)) * window
    return result


def weight_count(count):
    return smooth_axis(jnp.ones((count,), jnp.float32), 0, count)


def reference(density, mask):
    def one_plane(item):
        plane, level = item
        block_row = mask[level // CELLS]
        design_code = jnp.repeat(jnp.repeat(block_row, CELLS, 0), CELLS, 1)
        physical = jnp.where(design_code == 0, 0.0, jnp.where(design_code == 1, 1.0, plane))
        return smooth_axis(smooth_axis(physical, 1, NX), 0, NY)

    levels = jnp.arange(NZ, dtype=jnp.int32)
    flat = lax.map(one_plane, (density, levels))
    summed = smooth_axis(flat, 0, NZ)
    counts = weight_count(NZ)[:, None, None] * weight_count(NY)[None, :, None] * weight_count(NX)[None, None, :]
    filtered = summed / counts
    top = jnp.tanh(sharpness * threshold)
    projected = (top + jnp.tanh(sharpness * (filtered - threshold))) / (top + jnp.tanh(sharpness * (1.0 - threshold)))
    return filtered, projected
```

```python
import functools
import math

import jax
import jax.numpy as jnp
from jax import lax
from jax.experimental import pallas as pl
from jax.experimental.pallas import tpu as pltpu
from jax.sharding import PartitionSpec as P

RADIUS = 6
CELLS = 8
LANES = 128
SUBLANES = 8

sharpness = 8.0
threshold = 0.5
MESH = pl.DeviceIdType.MESH


def hat(rows, cols, offset):
    row = lax.broadcasted_iota(jnp.int32, (rows, cols), 0)
    col = lax.broadcasted_iota(jnp.int32, (rows, cols), 1)
    return jnp.maximum(RADIUS + 1 - jnp.abs(col + offset - row), 0).astype(jnp.float32)


def halves(values):
    high = values.astype(jnp.bfloat16)
    low = (values - high.astype(jnp.float32)).astype(jnp.bfloat16)
    return high, low


def projection(filtered):
    top = math.tanh(sharpness * threshold)
    bottom = top + math.tanh(sharpness * (1.0 - threshold))
    return (top + jnp.tanh(sharpness * (filtered - threshold))) * (1.0 / bottom)


def one_side(reach):
    return reach * (RADIUS + 1) - reach * (reach + 1) // 2


def dot(a, b):
    return jnp.dot(a, b, preferred_element_type=jnp.float32)


def x_filter(chunks, w_own, w_edge, xs, first):
    size, columns = chunks[0].shape
    high, low = zip(*[halves(chunk) for chunk in chunks])
    none = jnp.zeros((size, LANES), jnp.bfloat16)
    for c in range(len(chunks)):
        total = dot(high[c], w_own[...]) + dot(low[c], w_own[...])
        for part in (high, low):
            left = part[c - 1][:, columns - LANES :] if c > 0 else none
            right = part[c + 1][:, :LANES] if c < len(chunks) - 1 else none
            total = total + dot(jnp.concatenate([left, right], 1), w_edge[...])
        at = pl.ds(c * columns, columns)
        xs[pl.ds(first, size), at], xs[pl.ds(first + size, size), at] = halves(total)


def y_filter(xs, scale, scale_z, columns, put):
    rows, width = scale.shape
    own = hat(rows, rows, 0).astype(jnp.bfloat16)
    edge = jnp.concatenate([hat(rows, SUBLANES, -SUBLANES), hat(rows, SUBLANES, rows)], 1)
    edge = edge.astype(jnp.bfloat16)
    own = jnp.concatenate([own, own], 1)
    edge = jnp.concatenate([edge, edge], 1)
    for c in range(width // columns):
        at = pl.ds(c * columns, columns)
        summed = dot(own, xs[pl.ds(0, 2 * rows), at])
        summed = summed + dot(edge, xs[pl.ds(2 * rows, 4 * SUBLANES), at])
        put(at, summed * (scale[:, at] * scale_z))


def inverse_count(position, length):
    left = one_side(jnp.minimum(position, RADIUS))
    right = one_side(jnp.minimum(length - 1 - position, RADIUS))
    return 1.0 / (RADIUS + 1 + left + right).astype(jnp.float32)


def layer_of(k, layers):
    return jnp.where(lax.axis_index("gx") == 0, layers - 1 - k, k)


def scale_along_z(sizes, k, layers, columns):
    nz, nx, ny = sizes
    level = (lax.axis_index("gz") * nx + lax.axis_index("gx")) * layers + layer_of(k, layers)
    level = jnp.full((SUBLANES, columns), level, jnp.int32)
    return inverse_count(level, nz * nx * layers)[0:1]


def same(ref):
    return functools.partial(pltpu.make_async_copy, ref, ref)


def wait_sides(first, second, sem, one, both):
    @pl.when(jnp.logical_and(first, second))
    def _():
        same(both)(sem).wait()

    @pl.when(first != second)
    def _():
        same(one)(sem).wait()


def kernel(
    sizes,
    density,
    mask,
    fstage,
    pstage,
    lrecv,
    lyb,
    scale,
    w_own,
    w_edge,
    phys,
    codes,
    masks,
    zf,
    recv,
    yb,
    xs,
    load_sem,
    mask_sem,
    hmask_send,
    hmask_recv,
    halo_send,
    halo_recv,
    send_sem,
    recv_sem,
    y_send,
    y_recv,
    e_recv,
):
    nz, nx, ny = sizes
    planes, rows, columns = density.shape
    blocks, mrows, mcols = mask.shape
    layers = planes // nx
    final = layers - 1
    gz, gx, gy = lax.axis_index("gz"), lax.axis_index("gx"), lax.axis_index("gy")
    has_up, has_down = gz > 0, gz < nz - 1
    has_prev, has_next = gy > 0, gy < ny - 1

    def load(b):
        part = pl.ds(b * CELLS, CELLS)
        return pltpu.make_async_copy(
            density.at[part], phys.at[pl.ds(RADIUS + b * CELLS, CELLS)], load_sem.at[b]
        )

    mask_copy = pltpu.make_async_copy(mask, masks.at[pl.ds(1, blocks)], mask_sem)
    mask_copy.start()
    for b in range(blocks):
        load(b).start()

    barrier = pltpu.get_barrier_semaphore()

    def greet(**where):
        pl.semaphore_signal(barrier, inc=1, device_id=where, device_id_type=MESH)

    for step in range(1, nx):
        greet(gx=lax.rem(gx + step, nx))
    pl.when(has_up)(lambda: greet(gz=gz - 1))
    pl.when(has_down)(lambda: greet(gz=gz + 1))
    pl.when(has_prev)(lambda: greet(gy=gy - 1))
    pl.when(has_next)(lambda: greet(gy=gy + 1))

    def to_next(j):
        return pltpu.make_async_remote_copy(
            src_ref=density.at[planes - 1 - j],
            dst_ref=phys.at[RADIUS - 1 - j],
            send_sem=halo_send,
            recv_sem=halo_recv.at[j],
            device_id={"gz": gz + 1},
            device_id_type=MESH,
        )

    def to_previous(j):
        return pltpu.make_async_remote_copy(
            src_ref=density.at[j],
            dst_ref=phys.at[RADIUS + planes + j],
            send_sem=halo_send,
            recv_sem=halo_recv.at[j],
            device_id={"gz": gz - 1},
            device_id_type=MESH,
        )

    def mask_next():
        return pltpu.make_async_remote_copy(
            src_ref=mask.at[blocks - 1],
            dst_ref=masks.at[0],
            send_sem=hmask_send,
            recv_sem=hmask_recv,
            device_id={"gz": gz + 1},
            device_id_type=MESH,
        )

    def mask_previous():
        return pltpu.make_async_remote_copy(
            src_ref=mask.at[0],
            dst_ref=masks.at[blocks + 1],
            send_sem=hmask_send,
            recv_sem=hmask_recv,
            device_id={"gz": gz - 1},
            device_id_type=MESH,
        )

    def spread(b, count):
        small = masks[pl.ds(b, count)].reshape(count * mrows, mcols)
        small = small.astype(jnp.float32).astype(jnp.bfloat16)
        c = lax.broadcasted_iota(jnp.int32, (mcols, columns), 1) // CELLS
        n = lax.broadcasted_iota(jnp.int32, (mcols, columns), 0)
        wide = jnp.where(c == n, 1.0, 0.0).astype(jnp.bfloat16)
        codes[pl.ds(b * mrows, count * mrows)] = dot(small, wide)

    def apply_mask(row, count, b):
        def one(r, carry):
            at = pl.ds(pl.multiple_of(r * CELLS, CELLS), CELLS)
            code = jnp.broadcast_to(codes[pl.ds(b * mrows + r, 1)], (CELLS, columns))
            void, solid = code < 0.5, code < 1.5
            for i in range(count):
                held = phys[row + i, at]
                phys[row + i, at] = jnp.where(void, 0.0, jnp.where(solid, 1.0, held))
            return carry

        lax.fori_loop(0, mrows, one, 0, unroll=4 if count > 1 else 8)

    def piece(k, p, row):
        return pltpu.make_async_remote_copy(
            src_ref=zf.at[row],
            dst_ref=recv.at[k, gx],
            send_sem=send_sem,
            recv_sem=recv_sem.at[k],
            device_id={"gx": p},
            device_id_type=MESH,
        )

    edges = (pl.ds(0, SUBLANES), pl.ds(rows - SUBLANES, SUBLANES))
    inside = pl.ds(SUBLANES, rows - 2 * SUBLANES)

    def edge_piece(side, p, row):
        return pltpu.make_async_remote_copy(
            src_ref=zf.at[row, edges[side]],
            dst_ref=lrecv.at[gx, edges[side]],
            send_sem=send_sem,
            recv_sem=e_recv,
            device_id={"gx": p},
            device_id_type=MESH,
        )

    def inner_piece(p, row):
        return pltpu.make_async_remote_copy(
            src_ref=zf.at[row, inside],
            dst_ref=lrecv.at[gx, inside],
            send_sem=send_sem,
            recv_sem=recv_sem.at[final],
            device_id={"gx": p},
            device_id_type=MESH,
        )

    def row_of(k, p):
        return final - k if p == 0 else p * layers + k

    def z_filter(row, out):
        part = rows // 4
        for i in range(4):
            at = pl.ds(i * part, part)
            run = phys[row + RADIUS, at]
            total = run
            for d in range(1, RADIUS + 1):
                run = run + (phys[row + RADIUS - d, at] + phys[row + RADIUS + d, at])
                total = total + run
            out[at] = total

    def z_send(k, p):
        row = row_of(k, p)

        @pl.when(gx != p)
        def _():
            z_filter(row, zf.at[row])
            piece(k, p, row).start()

        @pl.when(gx == p)
        def _():
            z_filter(row, recv.at[k, p])

    def z_step(k, carry):
        for p in range(nx):
            z_send(k, p)
        return carry

    mask_copy.wait()
    spread(1, blocks)
    ready = 0
    for p in range(nx):
        need = min(blocks, (row_of(0, p) + RADIUS) // CELLS + 1)
        for b in range(ready, need):
            load(b).wait()
            apply_mask(RADIUS + b * CELLS, CELLS, b + 1)
        if p == 0:
            count = nx - 1
            for there in (has_up, has_down, has_prev, has_next):
                count = count + there.astype(jnp.int32)
            pl.semaphore_wait(barrier, count)
        ready = max(ready, need)
        z_send(0, p)
    for b in range(ready, blocks):
        load(b).wait()
        apply_mask(RADIUS + b * CELLS, CELLS, b + 1)

    @pl.when(has_down)
    def _():
        mask_next().start()
        for j in range(RADIUS):
            to_next(j).start()

    @pl.when(has_up)
    def _():
        mask_previous().start()
        for j in range(RADIUS):
            to_previous(j).start()

    free = layers - RADIUS
    lax.fori_loop(1, free, z_step, 0)

    @pl.when(jnp.logical_not(has_up))
    def _():
        phys[pl.ds(0, RADIUS)] = jnp.zeros((RADIUS, rows, columns), jnp.float32)

    @pl.when(jnp.logical_not(has_down))
    def _():
        phys[pl.ds(RADIUS + planes, RADIUS)] = jnp.zeros((RADIUS, rows, columns), jnp.float32)

    @pl.when(jnp.logical_not(has_prev))
    def _():
        lyb[:, pl.ds(0, SUBLANES)] = jnp.zeros((nx, SUBLANES, columns), jnp.float32)
        yb[:, :, pl.ds(0, SUBLANES)] = jnp.zeros((final, nx, SUBLANES, columns), jnp.float32)

    @pl.when(jnp.logical_not(has_next))
    def _():
        lyb[:, pl.ds(SUBLANES, SUBLANES)] = jnp.zeros((nx, SUBLANES, columns), jnp.float32)
        yb[:, :, pl.ds(SUBLANES, SUBLANES)] = jnp.zeros((final, nx, SUBLANES, columns), jnp.float32)

    w_own[...] = hat(columns, columns, 0).astype(jnp.bfloat16)
    w_edge[pl.ds(0, LANES)] = hat(LANES, columns, LANES).astype(jnp.bfloat16)
    w_edge[pl.ds(LANES, LANES)] = hat(LANES, columns, -columns).astype(jnp.bfloat16)

    width = nx * columns
    scale_y = inverse_count(
        gy * rows + lax.broadcasted_iota(jnp.int32, (rows, LANES), 0), rows * ny
    )
    for c in range(0, width, LANES):
        lane = c + lax.broadcasted_iota(jnp.int32, (SUBLANES, LANES), 1)
        scale_x = inverse_count(lane, width)
        scale[:, pl.ds(c, LANES)] = scale_y * scale_x[0:1]

    two = pl.ds(0, 2)
    wait_sides(has_up, has_down, hmask_send, masks.at[0], masks.at[two])
    wait_sides(has_up, has_down, hmask_recv, masks.at[0], masks.at[two])
    pl.when(has_up)(lambda: spread(0, 1))
    pl.when(has_down)(lambda: spread(blocks + 1, 1))

    def take_halo(k):
        j = k - free
        wait_sides(has_up, has_down, halo_recv.at[j], zf.at[0], zf.at[two])
        pl.when(has_up)(lambda: apply_mask(RADIUS - 1 - j, 1, 0))
        pl.when(has_down)(lambda: apply_mask(RADIUS + planes + j, 1, blocks + 1))

    def halo_step(k, carry):
        take_halo(k)
        return z_step(k, carry)

    lax.fori_loop(free, final, halo_step, 0)

    take_halo(final)
    for p in range(nx):
        row = row_of(final, p)

        @pl.when(gx != p)
        def _():
            z_filter(row, zf.at[row])
            edge_piece(0, p, row).start()
            edge_piece(1, p, row).start()

        @pl.when(gx == p)
        def _():
            z_filter(row, lrecv.at[p])

    for p in range(nx):

        @pl.when(gx != p)
        def _():
            inner_piece(p, row_of(final, p)).start()

    top, bottom = pl.ds(0, SUBLANES), pl.ds(SUBLANES, SUBLANES)

    def edge_to(where, k, held, side, landing, into):
        return pltpu.make_async_remote_copy(
            src_ref=held.at[:, edges[side]],
            dst_ref=landing.at[:, into],
            send_sem=y_send,
            recv_sem=y_recv.at[k],
            device_id={"gy": where},
            device_id_type=MESH,
        )

    def send_edges(k, held, landing):
        pl.when(has_prev)(lambda: edge_to(gy - 1, k, held, 0, landing, bottom).start())
        pl.when(has_next)(lambda: edge_to(gy + 1, k, held, 1, landing, top).start())

    def take_edges(k):
        wait_sides(has_prev, has_next, y_recv.at[k], lyb.at[:, top], lyb)

    def arrive(k):
        same(zf.at[pl.ds(0, nx - 1)])(recv_sem.at[k]).wait()
        send_edges(k, recv.at[k], yb.at[k])

    def process(k):
        x_filter([recv[k, c] for c in range(nx)], w_own, w_edge, xs, 0)
        take_edges(k)
        x_filter([yb[k, c] for c in range(nx)], w_own, w_edge, xs, 2 * rows)

        def put(at, value):
            fstage[k, :, at] = value
            pstage[k, :, at] = projection(value)

        y_filter(xs, scale, scale_along_z(sizes, k, layers, columns), columns, put)

    def take_step(k, carry):
        arrive(k)
        process(k - 1)
        return carry

    arrive(0)
    lax.fori_loop(1, final, take_step, 0)

    same(lrecv.at[pl.ds(0, nx - 1), pl.ds(0, 2 * SUBLANES)])(e_recv).wait()
    send_edges(final, lrecv, lyb)
    process(final - 1)

    half, whole = pl.ds(0, RADIUS), pl.ds(0, 2 * RADIUS)
    wait_sides(has_up, has_down, halo_send, zf.at[half], zf.at[whole])
    per_plane = columns * rows // (nx * SUBLANES * columns)
    half, whole = pl.ds(0, layers // per_plane), pl.ds(0, 2 * layers // per_plane)
    wait_sides(has_prev, has_next, y_send, zf.at[half], zf.at[whole])
    same(zf.at[pl.ds(0, (nx - 1) * layers)])(send_sem).wait()
    take_edges(final)
    same(lrecv.at[pl.ds(0, nx - 1), inside])(recv_sem.at[final]).wait()


def closing(sizes, fstage, pstage, lrecv, lyb, scale, w_own, w_edge, filt, proj, xs, flast, plast, sems):
    final = fstage.shape[0]
    nx, rows, columns = lrecv.shape
    layers = final + 1

    def finished(k, carry):
        at = layer_of(k, layers)
        pltpu.make_async_copy(fstage.at[k], filt.at[at], sems.at[0]).start()
        pltpu.make_async_copy(pstage.at[k], proj.at[at], sems.at[1]).start()
        return carry

    lax.fori_loop(0, final, finished, 0)
    x_filter([lrecv[c] for c in range(nx)], w_own, w_edge, xs, 0)
    x_filter([lyb[c] for c in range(nx)], w_own, w_edge, xs, 2 * rows)

    def put(at, value):
        flast[:, at] = value
        plast[:, at] = projection(value)

    y_filter(xs, scale, scale_along_z(sizes, final, layers, columns), columns, put)
    at = layer_of(final, layers)
    pltpu.make_async_copy(flast, filt.at[at], sems.at[0]).start()
    pltpu.make_async_copy(plast, proj.at[at], sems.at[1]).start()
    same(filt)(sems.at[0]).wait()
    same(proj)(sems.at[1]).wait()


def body(sizes, density, mask):
    planes, rows, columns = density.shape
    nz, nx, ny = sizes
    layers = planes // nx
    final = layers - 1
    blocks = mask.shape[0]
    width = nx * columns
    dma = pltpu.SemaphoreType.DMA
    f32, bf16 = jnp.float32, jnp.bfloat16
    shape = jax.ShapeDtypeStruct
    carried = (
        shape((final, rows, width), f32),
        shape((final, rows, width), f32),
        shape((nx, rows, columns), f32),
        shape((nx, 2 * SUBLANES, columns), f32),
        shape((rows, width), f32),
        shape((columns, columns), bf16),
        shape((2 * LANES, columns), bf16),
    )
    xs = pltpu.VMEM((2 * rows + 4 * SUBLANES, width), bf16)
    held = pl.pallas_call(
        functools.partial(kernel, sizes),
        out_shape=carried,
        in_specs=[pl.BlockSpec(memory_space=pltpu.HBM)] * 2,
        out_specs=(pl.BlockSpec(memory_space=pltpu.VMEM),) * len(carried),
        scratch_shapes=[
            pltpu.VMEM((planes + 2 * RADIUS, rows, columns), f32),
            pltpu.VMEM(((blocks + 2) * mask.shape[1], columns), f32),
            pltpu.VMEM((blocks + 2,) + mask.shape[1:], jnp.int32),
            pltpu.VMEM((planes, rows, columns), f32),
            pltpu.VMEM((final, nx, rows, columns), f32),
            pltpu.VMEM((final, nx, 2 * SUBLANES, columns), f32),
            xs,
            dma((blocks,)),
            dma,
            dma,
            dma,
            dma,
            dma((RADIUS,)),
            dma,
            dma((layers,)),
            dma,
            dma((layers,)),
            dma,
        ],
        compiler_params=pltpu.CompilerParams(
            collective_id=0, has_side_effects=True, vmem_limit_bytes=44 * 1024 * 1024
        ),
    )(density, pltpu.with_memory_space_constraint(mask, pltpu.HBM))
    return pl.pallas_call(
        functools.partial(closing, sizes),
        out_shape=(shape((layers, rows, width), f32),) * 2,
        in_specs=[pl.BlockSpec(memory_space=pltpu.VMEM)] * len(carried),
        out_specs=(pl.BlockSpec(memory_space=pl.ANY),) * 2,
        scratch_shapes=[
            xs,
            pltpu.VMEM((rows, width), f32),
            pltpu.VMEM((rows, width), f32),
            dma((2,)),
        ],
        compiler_params=pltpu.CompilerParams(vmem_limit_bytes=16 * 1024 * 1024),
    )(*held)


def solution(mesh):
    sizes = (mesh.shape["gz"], mesh.shape["gx"], mesh.shape["gy"])
    placed = (P("gz", "gy", "gx"), P("gz", "gy", "gx"))
    return jax.shard_map(
        functools.partial(body, sizes),
        mesh=mesh,
        in_specs=placed,
        out_specs=(P(("gz", "gx"), "gy", None), P(("gz", "gx"), "gy", None)),
        check_vma=False,
    )
```

```python
import functools
import math

import jax
import jax.numpy as jnp
from jax import lax
from jax.experimental import pallas as pl
from jax.experimental.pallas import tpu as pltpu
from jax.sharding import PartitionSpec as P

RADIUS = 6
CELLS = 8
LANES = 128
SUBLANES = 8

sharpness = 8.0
threshold = 0.5
MESH = pl.DeviceIdType.MESH


def hat(rows, cols, offset):
    row = lax.broadcasted_iota(jnp.int32, (rows, cols), 0)
    col = lax.broadcasted_iota(jnp.int32, (rows, cols), 1)
    return jnp.maximum(RADIUS + 1 - jnp.abs(col + offset - row), 0).astype(jnp.float32)


def halves(values):
    high = values.astype(jnp.bfloat16)
    low = (values - high.astype(jnp.float32)).astype(jnp.bfloat16)
    return high, low


def projection(filtered):
    top = math.tanh(sharpness * threshold)
    bottom = top + math.tanh(sharpness * (1.0 - threshold))
    return (top + jnp.tanh(sharpness * (filtered - threshold))) * (1.0 / bottom)


def one_side(reach):
    return reach * (RADIUS + 1) - reach * (reach + 1) // 2


def dot(a, b):
    return jnp.dot(a, b, preferred_element_type=jnp.float32)


def x_filter(chunks, w_own, w_edge, xs, first):
    size, columns = chunks[0].shape
    high, low = zip(*[halves(chunk) for chunk in chunks])
    none = jnp.zeros((size, LANES), jnp.bfloat16)
    for c in range(len(chunks)):
        total = dot(high[c], w_own[...]) + dot(low[c], w_own[...])
        for part in (high, low):
            left = part[c - 1][:, columns - LANES :] if c > 0 else none
            right = part[c + 1][:, :LANES] if c < len(chunks) - 1 else none
            total = total + dot(jnp.concatenate([left, right], 1), w_edge[...])
        at = pl.ds(c * columns, columns)
        xs[pl.ds(first, size), at], xs[pl.ds(first + size, size), at] = halves(total)


def y_filter(xs, scale, scale_z, columns, put):
    rows, width = scale.shape
    own = hat(rows, rows, 0).astype(jnp.bfloat16)
    edge = jnp.concatenate([hat(rows, SUBLANES, -SUBLANES), hat(rows, SUBLANES, rows)], 1)
    edge = edge.astype(jnp.bfloat16)
    own = jnp.concatenate([own, own], 1)
    edge = jnp.concatenate([edge, edge], 1)
    for c in range(width // columns):
        at = pl.ds(c * columns, columns)
        summed = dot(own, xs[pl.ds(0, 2 * rows), at])
        summed = summed + dot(edge, xs[pl.ds(2 * rows, 4 * SUBLANES), at])
        put(at, summed * (scale[:, at] * scale_z))


def inverse_count(position, length):
    left = one_side(jnp.minimum(position, RADIUS))
    right = one_side(jnp.minimum(length - 1 - position, RADIUS))
    return 1.0 / (RADIUS + 1 + left + right).astype(jnp.float32)


def layer_of(k, layers):
    return jnp.where(lax.axis_index("gx") == 0, layers - 1 - k, k)


def scale_along_z(sizes, k, layers, columns):
    nz, nx, ny = sizes
    level = (lax.axis_index("gz") * nx + lax.axis_index("gx")) * layers + layer_of(k, layers)
    level = jnp.full((SUBLANES, columns), level, jnp.int32)
    return inverse_count(level, nz * nx * layers)[0:1]


def same(ref):
    return functools.partial(pltpu.make_async_copy, ref, ref)


def wait_sides(first, second, sem, one, both):
    @pl.when(jnp.logical_and(first, second))
    def _():
        same(both)(sem).wait()

    @pl.when(first != second)
    def _():
        same(one)(sem).wait()


def kernel(
    sizes,
    density,
    mask,
    fstage,
    pstage,
    lrecv,
    lyb,
    scale,
    w_own,
    w_edge,
    phys,
    codes,
    masks,
    zf,
    recv,
    yb,
    xs,
    load_sem,
    mask_sem,
    hmask_send,
    hmask_recv,
    halo_send,
    halo_recv,
    send_sem,
    recv_sem,
    y_send,
    y_recv,
    e_recv,
    ready_x,
    ready_y,
    ready_z,
):
    nz, nx, ny = sizes
    planes, rows, columns = density.shape
    blocks, mrows, mcols = mask.shape
    layers = planes // nx
    final = layers - 1
    gz, gx, gy = lax.axis_index("gz"), lax.axis_index("gx"), lax.axis_index("gy")
    has_up, has_down = gz > 0, gz < nz - 1
    has_prev, has_next = gy > 0, gy < ny - 1
    odd = lax.rem(gy, 2) == 1
    sides = has_prev.astype(jnp.int32) + has_next.astype(jnp.int32)

    barrier = pltpu.get_barrier_semaphore()

    def greet(sem, **where):
        pl.semaphore_signal(sem, inc=1, device_id=where, device_id_type=MESH)

    later = tuple(lax.rem(gx + p, nx) for p in (3, 2, 1))
    order = tuple(p + (gx <= p).astype(jnp.int32) for p in range(nx - 1))

    def load(b):
        part = pl.ds(b * CELLS, CELLS)
        return pltpu.make_async_copy(
            density.at[part], phys.at[pl.ds(RADIUS + b * CELLS, CELLS)], load_sem.at[b]
        )

    mask_copy = pltpu.make_async_copy(mask, masks.at[pl.ds(1, blocks)], mask_sem)
    mask_copy.start()
    load(0).start()
    load(1).start()
    for p in range(1, nx):
        pl.when(gx < p)(lambda: greet(barrier, gx=p))
    pl.when(has_down)(lambda: greet(barrier, gz=gz + 1))
    pl.when(odd & has_next)(lambda: greet(barrier, gy=gy + 1))
    pl.when(odd)(lambda: greet(barrier, gy=gy - 1))
    for b in range(2, blocks):
        load(b).start()

    def to_next(j):
        return pltpu.make_async_remote_copy(
            src_ref=density.at[planes - 1 - j],
            dst_ref=phys.at[RADIUS - 1 - j],
            send_sem=halo_send,
            recv_sem=halo_recv.at[j],
            device_id={"gz": gz + 1},
            device_id_type=MESH,
        )

    def to_previous(j):
        return pltpu.make_async_remote_copy(
            src_ref=density.at[j],
            dst_ref=phys.at[RADIUS + planes + j],
            send_sem=halo_send,
            recv_sem=halo_recv.at[j],
            device_id={"gz": gz - 1},
            device_id_type=MESH,
        )

    def mask_next():
        return pltpu.make_async_remote_copy(
            src_ref=mask.at[blocks - 1],
            dst_ref=masks.at[0],
            send_sem=hmask_send,
            recv_sem=hmask_recv,
            device_id={"gz": gz + 1},
            device_id_type=MESH,
        )

    def mask_previous():
        return pltpu.make_async_remote_copy(
            src_ref=mask.at[0],
            dst_ref=masks.at[blocks + 1],
            send_sem=hmask_send,
            recv_sem=hmask_recv,
            device_id={"gz": gz - 1},
            device_id_type=MESH,
        )

    def spread(b, count):
        small = masks[pl.ds(b, count)].reshape(count * mrows, mcols)
        small = small.astype(jnp.float32).astype(jnp.bfloat16)
        c = lax.broadcasted_iota(jnp.int32, (mcols, columns), 1) // CELLS
        n = lax.broadcasted_iota(jnp.int32, (mcols, columns), 0)
        wide = jnp.where(c == n, 1.0, 0.0).astype(jnp.bfloat16)
        codes[pl.ds(b * mrows, count * mrows)] = dot(small, wide)

    def apply_mask(row, count, b):
        def one(r, carry):
            at = pl.ds(pl.multiple_of(r * CELLS, CELLS), CELLS)
            code = jnp.broadcast_to(codes[pl.ds(b * mrows + r, 1)], (CELLS, columns))
            void, solid = code < 0.5, code < 1.5
            for i in range(count):
                held = phys[row + i, at]
                phys[row + i, at] = jnp.where(void, 0.0, jnp.where(solid, 1.0, held))
            return carry

        lax.fori_loop(0, mrows, one, 0, unroll=4 if count > 1 else 8)

    def piece(k, p, row):
        return pltpu.make_async_remote_copy(
            src_ref=zf.at[row],
            dst_ref=recv.at[k, gx],
            send_sem=send_sem,
            recv_sem=recv_sem.at[k],
            device_id={"gx": p},
            device_id_type=MESH,
        )

    edges = (pl.ds(0, SUBLANES), pl.ds(rows - SUBLANES, SUBLANES))
    inside = pl.ds(SUBLANES, rows - 2 * SUBLANES)

    def part_piece(k, p, landing, part, sem):
        return pltpu.make_async_remote_copy(
            src_ref=zf.at[row_of(k, p), part],
            dst_ref=landing.at[gx, part],
            send_sem=send_sem,
            recv_sem=sem,
            device_id={"gx": p},
            device_id_type=MESH,
        )

    def row_of(k, p):
        return jnp.where(p == 0, final - k, p * layers + k)

    def z_filter(row, out):
        part = rows // 4
        for i in range(4):
            at = pl.ds(i * part, part)
            run = phys[row + RADIUS, at]
            total = run
            for d in range(1, RADIUS + 1):
                run = run + (phys[row + RADIUS - d, at] + phys[row + RADIUS + d, at])
                total = total + run
            out[at] = total

    def z_send(k, p):
        row = row_of(k, p)
        z_filter(row, zf.at[row])
        piece(k, p, row).start()

    def z_step(k, carry):
        for p in later:
            z_send(k, p)
        z_filter(row_of(k, gx), recv.at[k, gx])
        return carry

    def take_block(b):
        load(b).wait()
        apply_mask(RADIUS + b * CELLS, CELLS, b + 1)

    def ready(p):
        @pl.when(p > gx)
        def _():
            pl.semaphore_wait(ready_x.at[p], 1)

    earlier = gx + has_up.astype(jnp.int32) + jnp.where(odd, 0, sides)
    pl.when(earlier > 0)(lambda: pl.semaphore_wait(barrier, earlier))
    for p in range(nx - 1):
        pl.when(p < gx)(lambda: greet(ready_x.at[gx], gx=p))
    pl.when(has_up)(lambda: greet(ready_z, gz=gz - 1))
    pl.when(jnp.logical_not(odd) & has_prev)(lambda: greet(ready_y, gy=gy - 1))
    pl.when(jnp.logical_not(odd))(lambda: greet(ready_y, gy=gy + 1))
    mask_copy.wait()
    spread(1, blocks)
    take_block(0)
    take_block(1)
    ready(order[0])
    z_send(0, order[0])
    pl.when(gx > 1)(lambda: z_send(0, order[1]))
    for b in range(2, blocks):
        take_block(b)

    @pl.when(gx <= 1)
    def _():
        ready(order[1])
        z_send(0, order[1])

    for p in order[2:]:
        ready(p)
        z_send(0, p)
    z_filter(row_of(0, gx), recv.at[0, gx])

    @pl.when(has_up)
    def _():
        mask_previous().start()
        for j in range(RADIUS):
            to_previous(j).start()

    @pl.when(has_down)
    def _():
        pl.semaphore_wait(ready_z, 1)
        mask_next().start()
        for j in range(RADIUS):
            to_next(j).start()

    pl.when(odd)(lambda: pl.semaphore_wait(ready_y, sides))

    free = layers - RADIUS
    lax.fori_loop(1, free, z_step, 0)

    @pl.when(jnp.logical_not(has_up))
    def _():
        phys[pl.ds(0, RADIUS)] = jnp.zeros((RADIUS, rows, columns), jnp.float32)

    @pl.when(jnp.logical_not(has_down))
    def _():
        phys[pl.ds(RADIUS + planes, RADIUS)] = jnp.zeros((RADIUS, rows, columns), jnp.float32)

    @pl.when(jnp.logical_not(has_prev))
    def _():
        lyb[:, pl.ds(0, SUBLANES)] = jnp.zeros((nx, SUBLANES, columns), jnp.float32)
        yb[:, :, pl.ds(0, SUBLANES)] = jnp.zeros((final, nx, SUBLANES, columns), jnp.float32)

    @pl.when(jnp.logical_not(has_next))
    def _():
        lyb[:, pl.ds(SUBLANES, SUBLANES)] = jnp.zeros((nx, SUBLANES, columns), jnp.float32)
        yb[:, :, pl.ds(SUBLANES, SUBLANES)] = jnp.zeros((final, nx, SUBLANES, columns), jnp.float32)

    w_own[...] = hat(columns, columns, 0).astype(jnp.bfloat16)
    w_edge[pl.ds(0, LANES)] = hat(LANES, columns, LANES).astype(jnp.bfloat16)
    w_edge[pl.ds(LANES, LANES)] = hat(LANES, columns, -columns).astype(jnp.bfloat16)

    width = nx * columns
    scale_y = inverse_count(
        gy * rows + lax.broadcasted_iota(jnp.int32, (rows, LANES), 0), rows * ny
    )
    for c in range(0, width, LANES):
        lane = c + lax.broadcasted_iota(jnp.int32, (SUBLANES, LANES), 1)
        scale_x = inverse_count(lane, width)
        scale[:, pl.ds(c, LANES)] = scale_y * scale_x[0:1]

    two = pl.ds(0, 2)
    wait_sides(has_up, has_down, hmask_send, masks.at[0], masks.at[two])
    wait_sides(has_up, has_down, hmask_recv, masks.at[0], masks.at[two])
    pl.when(has_up)(lambda: spread(0, 1))
    pl.when(has_down)(lambda: spread(blocks + 1, 1))

    def take_halo(k):
        j = k - free
        wait_sides(has_up, has_down, halo_recv.at[j], zf.at[0], zf.at[two])
        pl.when(has_up)(lambda: apply_mask(RADIUS - 1 - j, 1, 0))
        pl.when(has_down)(lambda: apply_mask(RADIUS + planes + j, 1, blocks + 1))

    def halo_step(k, carry):
        take_halo(k)
        return z_step(k, carry)

    before = final - 1
    lax.fori_loop(free, before, halo_step, 0)

    last = ((before, recv.at[before]), (final, lrecv))
    for k, landing in last:
        take_halo(k)
        for p in later:
            z_filter(row_of(k, p), zf.at[row_of(k, p)])
        z_filter(row_of(k, gx), landing.at[gx])
    for k, landing in last:
        for p in later:
            for side in edges:
                part_piece(k, p, landing, side, e_recv).start()
    for k, landing in last:
        for p in later:
            part_piece(k, p, landing, inside, recv_sem.at[k]).start()

    top, bottom = pl.ds(0, SUBLANES), pl.ds(SUBLANES, SUBLANES)

    def edge_to(where, k, held, side, landing, into):
        return pltpu.make_async_remote_copy(
            src_ref=held.at[:, edges[side]],
            dst_ref=landing.at[:, into],
            send_sem=y_send,
            recv_sem=y_recv.at[k],
            device_id={"gy": where},
            device_id_type=MESH,
        )

    def send_edges(k, held, landing):
        pl.when(has_prev)(lambda: edge_to(gy - 1, k, held, 0, landing, bottom).start())
        pl.when(has_next)(lambda: edge_to(gy + 1, k, held, 1, landing, top).start())

    def take_edges(k):
        wait_sides(has_prev, has_next, y_recv.at[k], lyb.at[:, top], lyb)

    def arrive(k):
        same(zf.at[pl.ds(0, nx - 1)])(recv_sem.at[k]).wait()
        send_edges(k, recv.at[k], yb.at[k])

    def process(k):
        x_filter([recv[k, c] for c in range(nx)], w_own, w_edge, xs, 0)
        take_edges(k)
        x_filter([yb[k, c] for c in range(nx)], w_own, w_edge, xs, 2 * rows)

        def put(at, value):
            fstage[k, :, at] = value
            pstage[k, :, at] = projection(value)

        y_filter(xs, scale, scale_along_z(sizes, k, layers, columns), columns, put)

    def take_step(k, carry):
        arrive(k)
        process(k - 1)
        return carry

    def inner(k):
        same(lrecv.at[pl.ds(0, nx - 1), inside])(recv_sem.at[k]).wait()

    arrive(0)
    lax.fori_loop(1, before, take_step, 0)

    same(lrecv.at[pl.ds(0, nx - 1), pl.ds(0, 4 * SUBLANES)])(e_recv).wait()
    send_edges(before, recv.at[before], yb.at[before])
    send_edges(final, lrecv, lyb)
    process(before - 1)
    inner(before)
    process(before)

    half, whole = pl.ds(0, RADIUS), pl.ds(0, 2 * RADIUS)
    wait_sides(has_up, has_down, halo_send, zf.at[half], zf.at[whole])
    per_plane = columns * rows // (nx * SUBLANES * columns)
    half, whole = pl.ds(0, layers // per_plane), pl.ds(0, 2 * layers // per_plane)
    wait_sides(has_prev, has_next, y_send, zf.at[half], zf.at[whole])
    same(zf.at[pl.ds(0, (nx - 1) * layers)])(send_sem).wait()
    take_edges(final)
    inner(final)


def closing(sizes, fstage, pstage, lrecv, lyb, scale, w_own, w_edge, filt, proj, xs, flast, plast, sems):
    final = fstage.shape[0]
    nx, rows, columns = lrecv.shape
    layers = final + 1

    def finished(k, carry):
        at = layer_of(k, layers)
        pltpu.make_async_copy(fstage.at[k], filt.at[at], sems.at[0]).start()
        pltpu.make_async_copy(pstage.at[k], proj.at[at], sems.at[1]).start()
        return carry

    lax.fori_loop(0, final, finished, 0)
    x_filter([lrecv[c] for c in range(nx)], w_own, w_edge, xs, 0)
    x_filter([lyb[c] for c in range(nx)], w_own, w_edge, xs, 2 * rows)

    def put(at, value):
        flast[:, at] = value
        plast[:, at] = projection(value)

    y_filter(xs, scale, scale_along_z(sizes, final, layers, columns), columns, put)
    at = layer_of(final, layers)
    pltpu.make_async_copy(flast, filt.at[at], sems.at[0]).start()
    pltpu.make_async_copy(plast, proj.at[at], sems.at[1]).start()
    same(filt)(sems.at[0]).wait()
    same(proj)(sems.at[1]).wait()


def body(sizes, density, mask):
    planes, rows, columns = density.shape
    nz, nx, ny = sizes
    layers = planes // nx
    final = layers - 1
    blocks = mask.shape[0]
    width = nx * columns
    dma = pltpu.SemaphoreType.DMA
    f32, bf16 = jnp.float32, jnp.bfloat16
    shape = jax.ShapeDtypeStruct
    carried = (
        shape((final, rows, width), f32),
        shape((final, rows, width), f32),
        shape((nx, rows, columns), f32),
        shape((nx, 2 * SUBLANES, columns), f32),
        shape((rows, width), f32),
        shape((columns, columns), bf16),
        shape((2 * LANES, columns), bf16),
    )
    xs = pltpu.VMEM((2 * rows + 4 * SUBLANES, width), bf16)
    held = pl.pallas_call(
        functools.partial(kernel, sizes),
        out_shape=carried,
        in_specs=[pl.BlockSpec(memory_space=pltpu.HBM)] * 2,
        out_specs=(pl.BlockSpec(memory_space=pltpu.VMEM),) * len(carried),
        scratch_shapes=[
            pltpu.VMEM((planes + 2 * RADIUS, rows, columns), f32),
            pltpu.VMEM(((blocks + 2) * mask.shape[1], columns), f32),
            pltpu.VMEM((blocks + 2,) + mask.shape[1:], jnp.int32),
            pltpu.VMEM((planes, rows, columns), f32),
            pltpu.VMEM((final, nx, rows, columns), f32),
            pltpu.VMEM((final, nx, 2 * SUBLANES, columns), f32),
            xs,
            dma((blocks,)),
            dma,
            dma,
            dma,
            dma,
            dma((RADIUS,)),
            dma,
            dma((layers,)),
            dma,
            dma((layers,)),
            dma,
            pltpu.SemaphoreType.REGULAR((nx,)),
            pltpu.SemaphoreType.REGULAR,
            pltpu.SemaphoreType.REGULAR,
        ],
        compiler_params=pltpu.CompilerParams(
            collective_id=0, has_side_effects=True, vmem_limit_bytes=44 * 1024 * 1024
        ),
    )(density, pltpu.with_memory_space_constraint(mask, pltpu.HBM))
    return pl.pallas_call(
        functools.partial(closing, sizes),
        out_shape=(shape((layers, rows, width), f32),) * 2,
        in_specs=[pl.BlockSpec(memory_space=pltpu.VMEM)] * len(carried),
        out_specs=(pl.BlockSpec(memory_space=pl.ANY),) * 2,
        scratch_shapes=[
            xs,
            pltpu.VMEM((rows, width), f32),
            pltpu.VMEM((rows, width), f32),
            dma((2,)),
        ],
        compiler_params=pltpu.CompilerParams(vmem_limit_bytes=16 * 1024 * 1024),
    )(*held)


def solution(mesh):
    sizes = (mesh.shape["gz"], mesh.shape["gx"], mesh.shape["gy"])
    placed = (P("gz", "gy", "gx"), P("gz", "gy", "gx"))
    return jax.shard_map(
        functools.partial(body, sizes),
        mesh=mesh,
        in_specs=placed,
        out_specs=(P(("gz", "gx"), "gy", None), P(("gz", "gx"), "gy", None)),
        check_vma=False,
    )
```

```python
import functools
import math

import jax
import jax.numpy as jnp
from jax import lax
from jax.experimental import pallas as pl
from jax.experimental.pallas import tpu as pltpu
from jax.sharding import PartitionSpec as P

RADIUS = 6
CELLS = 8
LANES = 128
SUBLANES = 8

sharpness = 8.0
threshold = 0.5
MESH = pl.DeviceIdType.MESH


def hat(rows, cols, offset):
    row = lax.broadcasted_iota(jnp.int32, (rows, cols), 0)
    col = lax.broadcasted_iota(jnp.int32, (rows, cols), 1)
    return jnp.maximum(RADIUS + 1 - jnp.abs(col + offset - row), 0).astype(jnp.float32)


def halves(values):
    high = values.astype(jnp.bfloat16)
    low = (values - high.astype(jnp.float32)).astype(jnp.bfloat16)
    return high, low


def projection(filtered):
    top = math.tanh(sharpness * threshold)
    bottom = top + math.tanh(sharpness * (1.0 - threshold))
    return (top + jnp.tanh(sharpness * (filtered - threshold))) * (1.0 / bottom)


def one_side(reach):
    return reach * (RADIUS + 1) - reach * (reach + 1) // 2


def dot(a, b):
    return jnp.dot(a, b, preferred_element_type=jnp.float32)


def x_filter(chunks, w_own, w_edge, xs, first):
    size, columns = chunks[0].shape
    high, low = zip(*[halves(chunk) for chunk in chunks])
    none = jnp.zeros((size, LANES), jnp.bfloat16)
    for c in range(len(chunks)):
        total = dot(high[c], w_own[...]) + dot(low[c], w_own[...])
        for part in (high, low):
            left = part[c - 1][:, columns - LANES :] if c > 0 else none
            right = part[c + 1][:, :LANES] if c < len(chunks) - 1 else none
            total = total + dot(jnp.concatenate([left, right], 1), w_edge[...])
        at = pl.ds(c * columns, columns)
        xs[pl.ds(first, size), at], xs[pl.ds(first + size, size), at] = halves(total)


def y_filter(xs, scale, scale_z, columns, put):
    rows, width = scale.shape
    own = hat(rows, rows, 0).astype(jnp.bfloat16)
    edge = jnp.concatenate([hat(rows, SUBLANES, -SUBLANES), hat(rows, SUBLANES, rows)], 1)
    edge = edge.astype(jnp.bfloat16)
    own = jnp.concatenate([own, own], 1)
    edge = jnp.concatenate([edge, edge], 1)
    for c in range(width // columns):
        at = pl.ds(c * columns, columns)
        summed = dot(own, xs[pl.ds(0, 2 * rows), at])
        summed = summed + dot(edge, xs[pl.ds(2 * rows, 4 * SUBLANES), at])
        put(at, summed * (scale[:, at] * scale_z))


def inverse_count(position, length):
    left = one_side(jnp.minimum(position, RADIUS))
    right = one_side(jnp.minimum(length - 1 - position, RADIUS))
    return 1.0 / (RADIUS + 1 + left + right).astype(jnp.float32)


def layer_of(k, layers):
    return jnp.where(lax.axis_index("gx") == 0, layers - 1 - k, k)


def scale_along_z(sizes, k, layers, columns):
    nz, nx, ny = sizes
    level = (lax.axis_index("gz") * nx + lax.axis_index("gx")) * layers + layer_of(k, layers)
    level = jnp.full((SUBLANES, columns), level, jnp.int32)
    return inverse_count(level, nz * nx * layers)[0:1]


def same(ref):
    return functools.partial(pltpu.make_async_copy, ref, ref)


def wait_sides(first, second, sem, one, both):
    @pl.when(jnp.logical_and(first, second))
    def _():
        same(both)(sem).wait()

    @pl.when(first != second)
    def _():
        same(one)(sem).wait()


def kernel(
    sizes,
    density,
    mask,
    fstage,
    pstage,
    lrecv,
    lyb,
    scale,
    w_own,
    w_edge,
    phys,
    codes,
    masks,
    zf,
    recv,
    yb,
    xs,
    load_sem,
    part_sem,
    mask_sem,
    hmask_send,
    hmask_recv,
    halo_send,
    halo_recv,
    send_sem,
    recv_sem,
    y_send,
    y_recv,
    e_recv,
    ready_y,
    ready_z,
):
    nz, nx, ny = sizes
    planes, rows, columns = density.shape
    blocks, mrows, mcols = mask.shape
    layers = planes // nx
    final = layers - 1
    gz, gx, gy = lax.axis_index("gz"), lax.axis_index("gx"), lax.axis_index("gy")
    has_up, has_down = gz > 0, gz < nz - 1
    has_prev, has_next = gy > 0, gy < ny - 1
    odd = lax.rem(gy, 2) == 1
    sides = has_prev.astype(jnp.int32) + has_next.astype(jnp.int32)

    barrier = pltpu.get_barrier_semaphore()

    def greet(sem, **where):
        pl.semaphore_signal(sem, inc=1, device_id=where, device_id_type=MESH)

    later = tuple(lax.rem(gx + p, nx) for p in (3, 2, 1))
    ahead = 2
    parts = 4
    part_rows = rows // parts

    def rows_of(q):
        return pl.ds(pl.multiple_of(q * part_rows, part_rows), part_rows)

    def load_part(q):
        return pltpu.make_async_copy(
            density.at[pl.ds(0, ahead * CELLS), rows_of(q)],
            phys.at[pl.ds(RADIUS, ahead * CELLS), rows_of(q)],
            part_sem.at[q],
        )

    def load(b):
        part = pl.ds(b * CELLS, CELLS)
        return pltpu.make_async_copy(
            density.at[part], phys.at[pl.ds(RADIUS + b * CELLS, CELLS)], load_sem.at[b - ahead]
        )

    for step in (2, 1, 3):
        greet(barrier, gx=lax.rem(gx + step, nx))
    mask_copy = pltpu.make_async_copy(mask, masks.at[pl.ds(1, blocks)], mask_sem)
    mask_copy.start()
    load_part(0).start()
    pl.when(has_down)(lambda: greet(barrier, gz=gz + 1))
    pl.when(odd & has_next)(lambda: greet(barrier, gy=gy + 1))
    pl.when(odd)(lambda: greet(barrier, gy=gy - 1))
    for q in range(1, parts):
        load_part(q).start()
    for b in range(ahead, blocks):
        load(b).start()

    def to_next(j):
        return pltpu.make_async_remote_copy(
            src_ref=density.at[planes - 1 - j],
            dst_ref=phys.at[RADIUS - 1 - j],
            send_sem=halo_send,
            recv_sem=halo_recv.at[j],
            device_id={"gz": gz + 1},
            device_id_type=MESH,
        )

    def to_previous(j):
        return pltpu.make_async_remote_copy(
            src_ref=density.at[j],
            dst_ref=phys.at[RADIUS + planes + j],
            send_sem=halo_send,
            recv_sem=halo_recv.at[j],
            device_id={"gz": gz - 1},
            device_id_type=MESH,
        )

    def mask_next():
        return pltpu.make_async_remote_copy(
            src_ref=mask.at[blocks - 1],
            dst_ref=masks.at[0],
            send_sem=hmask_send,
            recv_sem=hmask_recv,
            device_id={"gz": gz + 1},
            device_id_type=MESH,
        )

    def mask_previous():
        return pltpu.make_async_remote_copy(
            src_ref=mask.at[0],
            dst_ref=masks.at[blocks + 1],
            send_sem=hmask_send,
            recv_sem=hmask_recv,
            device_id={"gz": gz - 1},
            device_id_type=MESH,
        )

    def spread(b, count):
        small = masks[pl.ds(b, count)].reshape(count * mrows, mcols)
        small = small.astype(jnp.float32).astype(jnp.bfloat16)
        c = lax.broadcasted_iota(jnp.int32, (mcols, columns), 1) // CELLS
        n = lax.broadcasted_iota(jnp.int32, (mcols, columns), 0)
        wide = jnp.where(c == n, 1.0, 0.0).astype(jnp.bfloat16)
        codes[pl.ds(b * mrows, count * mrows)] = dot(small, wide)

    def apply_rows(row, count, b, r):
        at = pl.ds(pl.multiple_of(r * CELLS, CELLS), CELLS)
        code = jnp.broadcast_to(codes[pl.ds(b * mrows + r, 1)], (CELLS, columns))
        void, solid = code < 0.5, code < 1.5
        for i in range(count):
            held = phys[row + i, at]
            phys[row + i, at] = jnp.where(void, 0.0, jnp.where(solid, 1.0, held))

    def apply_mask(row, count, b):
        def one(r, carry):
            apply_rows(row, count, b, r)
            return carry

        lax.fori_loop(0, mrows, one, 0, unroll=4 if count > 1 else 8)

    def first_piece(p, row, at):
        return pltpu.make_async_remote_copy(
            src_ref=zf.at[row, at],
            dst_ref=recv.at[0, gx, at],
            send_sem=send_sem,
            recv_sem=recv_sem.at[0],
            device_id={"gx": p},
            device_id_type=MESH,
        )

    def piece(k, p, row):
        return pltpu.make_async_remote_copy(
            src_ref=zf.at[row],
            dst_ref=recv.at[k, gx],
            send_sem=send_sem,
            recv_sem=recv_sem.at[k],
            device_id={"gx": p},
            device_id_type=MESH,
        )

    edges = (pl.ds(0, SUBLANES), pl.ds(rows - SUBLANES, SUBLANES))
    inside = pl.ds(SUBLANES, rows - 2 * SUBLANES)

    def part_piece(k, p, landing, part, sem):
        return pltpu.make_async_remote_copy(
            src_ref=zf.at[row_of(k, p), part],
            dst_ref=landing.at[gx, part],
            send_sem=send_sem,
            recv_sem=sem,
            device_id={"gx": p},
            device_id_type=MESH,
        )

    def row_of(k, p):
        if isinstance(p, int):
            return final - k if p == 0 else p * layers + k
        return jnp.where(p == 0, final - k, p * layers + k)

    def z_part(row, at, out):
        run = phys[row + RADIUS, at]
        total = run
        for d in range(1, RADIUS + 1):
            run = run + (phys[row + RADIUS - d, at] + phys[row + RADIUS + d, at])
            total = total + run
        out[at] = total

    def z_filter(row, out):
        for q in range(parts):
            z_part(row, pl.ds(q * part_rows, part_rows), out)

    def z_send(k, p):
        row = row_of(k, p)
        z_filter(row, zf.at[row])
        piece(k, p, row).start()

    def z_step(k, carry):
        for p in later:
            z_send(k, p)
        z_filter(row_of(k, gx), recv.at[k, gx])
        return carry

    def first_part(q, carry):
        at = rows_of(q)
        load_part(q).wait()
        for b in range(ahead):
            for r in range(mrows // parts):
                apply_rows(RADIUS + b * CELLS, CELLS, b + 1, q * (mrows // parts) + r)
        for p in range(ahead):
            row = row_of(0, p)

            @pl.when(gx != p)
            def _():
                z_part(row, at, zf.at[row])
                first_piece(p, row, at).start()

            @pl.when(gx == p)
            def _():
                z_part(row, at, recv.at[0, p])

        return carry

    mask_copy.wait()
    spread(1, blocks)
    pl.semaphore_wait(barrier, nx - 1 + has_up.astype(jnp.int32) + jnp.where(odd, 0, sides))
    lax.fori_loop(0, parts, first_part, 0)
    for b in range(ahead, blocks):
        load(b).wait()
        apply_mask(RADIUS + b * CELLS, CELLS, b + 1)
    for p in range(ahead, nx):
        pl.when(gx != p)(lambda: z_send(0, p))
        pl.when(gx == p)(lambda: z_filter(row_of(0, p), recv.at[0, p]))
    pl.when(has_up)(lambda: greet(ready_z, gz=gz - 1))
    pl.when(jnp.logical_not(odd) & has_prev)(lambda: greet(ready_y, gy=gy - 1))
    pl.when(jnp.logical_not(odd))(lambda: greet(ready_y, gy=gy + 1))

    @pl.when(has_up)
    def _():
        mask_previous().start()
        for j in range(RADIUS):
            to_previous(j).start()

    free = layers - RADIUS
    lax.fori_loop(1, free, z_step, 0)

    @pl.when(has_down)
    def _():
        pl.semaphore_wait(ready_z, 1)
        mask_next().start()
        for j in range(RADIUS):
            to_next(j).start()

    pl.when(odd)(lambda: pl.semaphore_wait(ready_y, sides))

    @pl.when(jnp.logical_not(has_up))
    def _():
        phys[pl.ds(0, RADIUS)] = jnp.zeros((RADIUS, rows, columns), jnp.float32)

    @pl.when(jnp.logical_not(has_down))
    def _():
        phys[pl.ds(RADIUS + planes, RADIUS)] = jnp.zeros((RADIUS, rows, columns), jnp.float32)

    @pl.when(jnp.logical_not(has_prev))
    def _():
        lyb[:, pl.ds(0, SUBLANES)] = jnp.zeros((nx, SUBLANES, columns), jnp.float32)
        yb[:, :, pl.ds(0, SUBLANES)] = jnp.zeros((final, nx, SUBLANES, columns), jnp.float32)

    @pl.when(jnp.logical_not(has_next))
    def _():
        lyb[:, pl.ds(SUBLANES, SUBLANES)] = jnp.zeros((nx, SUBLANES, columns), jnp.float32)
        yb[:, :, pl.ds(SUBLANES, SUBLANES)] = jnp.zeros((final, nx, SUBLANES, columns), jnp.float32)

    w_own[...] = hat(columns, columns, 0).astype(jnp.bfloat16)
    w_edge[pl.ds(0, LANES)] = hat(LANES, columns, LANES).astype(jnp.bfloat16)
    w_edge[pl.ds(LANES, LANES)] = hat(LANES, columns, -columns).astype(jnp.bfloat16)

    width = nx * columns
    scale_y = inverse_count(
        gy * rows + lax.broadcasted_iota(jnp.int32, (rows, LANES), 0), rows * ny
    )
    for c in range(0, width, LANES):
        lane = c + lax.broadcasted_iota(jnp.int32, (SUBLANES, LANES), 1)
        scale_x = inverse_count(lane, width)
        scale[:, pl.ds(c, LANES)] = scale_y * scale_x[0:1]

    two = pl.ds(0, 2)
    wait_sides(has_up, has_down, hmask_send, masks.at[0], masks.at[two])
    wait_sides(has_up, has_down, hmask_recv, masks.at[0], masks.at[two])
    pl.when(has_up)(lambda: spread(0, 1))
    pl.when(has_down)(lambda: spread(blocks + 1, 1))

    def take_halo(k):
        j = k - free
        wait_sides(has_up, has_down, halo_recv.at[j], zf.at[0], zf.at[two])
        pl.when(has_up)(lambda: apply_mask(RADIUS - 1 - j, 1, 0))
        pl.when(has_down)(lambda: apply_mask(RADIUS + planes + j, 1, blocks + 1))

    def halo_step(k, carry):
        take_halo(k)
        return z_step(k, carry)

    before = final - 1
    lax.fori_loop(free, before, halo_step, 0)

    last = ((before, recv.at[before]), (final, lrecv))
    for k, landing in last:
        take_halo(k)
        for p in later:
            z_filter(row_of(k, p), zf.at[row_of(k, p)])
        z_filter(row_of(k, gx), landing.at[gx])
    for k, landing in last:
        for p in later:
            for side in edges:
                part_piece(k, p, landing, side, e_recv).start()
    for k, landing in last:
        for p in later:
            part_piece(k, p, landing, inside, recv_sem.at[k]).start()

    top, bottom = pl.ds(0, SUBLANES), pl.ds(SUBLANES, SUBLANES)

    def edge_to(where, k, held, side, landing, into):
        return pltpu.make_async_remote_copy(
            src_ref=held.at[:, edges[side]],
            dst_ref=landing.at[:, into],
            send_sem=y_send,
            recv_sem=y_recv.at[k],
            device_id={"gy": where},
            device_id_type=MESH,
        )

    def send_edges(k, held, landing):
        pl.when(has_prev)(lambda: edge_to(gy - 1, k, held, 0, landing, bottom).start())
        pl.when(has_next)(lambda: edge_to(gy + 1, k, held, 1, landing, top).start())

    def take_edges(k):
        wait_sides(has_prev, has_next, y_recv.at[k], lyb.at[:, top], lyb)

    def arrive(k):
        same(zf.at[pl.ds(0, nx - 1)])(recv_sem.at[k]).wait()
        send_edges(k, recv.at[k], yb.at[k])

    def process(k):
        x_filter([recv[k, c] for c in range(nx)], w_own, w_edge, xs, 0)
        take_edges(k)
        x_filter([yb[k, c] for c in range(nx)], w_own, w_edge, xs, 2 * rows)

        def put(at, value):
            fstage[k, :, at] = value
            pstage[k, :, at] = projection(value)

        y_filter(xs, scale, scale_along_z(sizes, k, layers, columns), columns, put)

    def take_step(k, carry):
        arrive(k)
        process(k - 1)
        return carry

    def inner(k):
        same(lrecv.at[pl.ds(0, nx - 1), inside])(recv_sem.at[k]).wait()

    arrive(0)
    lax.fori_loop(1, before, take_step, 0)

    same(lrecv.at[pl.ds(0, nx - 1), pl.ds(0, 4 * SUBLANES)])(e_recv).wait()
    send_edges(before, recv.at[before], yb.at[before])
    send_edges(final, lrecv, lyb)
    process(before - 1)
    inner(before)
    process(before)

    half, whole = pl.ds(0, RADIUS), pl.ds(0, 2 * RADIUS)
    wait_sides(has_up, has_down, halo_send, zf.at[half], zf.at[whole])
    per_plane = columns * rows // (nx * SUBLANES * columns)
    half, whole = pl.ds(0, layers // per_plane), pl.ds(0, 2 * layers // per_plane)
    wait_sides(has_prev, has_next, y_send, zf.at[half], zf.at[whole])
    same(zf.at[pl.ds(0, (nx - 1) * layers)])(send_sem).wait()
    take_edges(final)
    inner(final)


def closing(sizes, fstage, pstage, lrecv, lyb, scale, w_own, w_edge, filt, proj, xs, flast, plast, sems):
    final = fstage.shape[0]
    nx, rows, columns = lrecv.shape
    layers = final + 1

    def finished(k, carry):
        at = layer_of(k, layers)
        pltpu.make_async_copy(fstage.at[k], filt.at[at], sems.at[0]).start()
        pltpu.make_async_copy(pstage.at[k], proj.at[at], sems.at[1]).start()
        return carry

    lax.fori_loop(0, final, finished, 0)
    x_filter([lrecv[c] for c in range(nx)], w_own, w_edge, xs, 0)
    x_filter([lyb[c] for c in range(nx)], w_own, w_edge, xs, 2 * rows)

    def put(at, value):
        flast[:, at] = value
        plast[:, at] = projection(value)

    y_filter(xs, scale, scale_along_z(sizes, final, layers, columns), columns, put)
    at = layer_of(final, layers)
    pltpu.make_async_copy(flast, filt.at[at], sems.at[0]).start()
    pltpu.make_async_copy(plast, proj.at[at], sems.at[1]).start()
    same(filt)(sems.at[0]).wait()
    same(proj)(sems.at[1]).wait()


def body(sizes, density, mask):
    planes, rows, columns = density.shape
    nz, nx, ny = sizes
    layers = planes // nx
    final = layers - 1
    blocks = mask.shape[0]
    width = nx * columns
    dma = pltpu.SemaphoreType.DMA
    f32, bf16 = jnp.float32, jnp.bfloat16
    shape = jax.ShapeDtypeStruct
    carried = (
        shape((final, rows, width), f32),
        shape((final, rows, width), f32),
        shape((nx, rows, columns), f32),
        shape((nx, 2 * SUBLANES, columns), f32),
        shape((rows, width), f32),
        shape((columns, columns), bf16),
        shape((2 * LANES, columns), bf16),
    )
    xs = pltpu.VMEM((2 * rows + 4 * SUBLANES, width), bf16)
    held = pl.pallas_call(
        functools.partial(kernel, sizes),
        out_shape=carried,
        in_specs=[pl.BlockSpec(memory_space=pltpu.HBM)] * 2,
        out_specs=(pl.BlockSpec(memory_space=pltpu.VMEM),) * len(carried),
        scratch_shapes=[
            pltpu.VMEM((planes + 2 * RADIUS, rows, columns), f32),
            pltpu.VMEM(((blocks + 2) * mask.shape[1], columns), f32),
            pltpu.VMEM((blocks + 2,) + mask.shape[1:], jnp.int32),
            pltpu.VMEM((planes, rows, columns), f32),
            pltpu.VMEM((final, nx, rows, columns), f32),
            pltpu.VMEM((final, nx, 2 * SUBLANES, columns), f32),
            xs,
            dma((blocks - 2,)),
            dma((4,)),
            dma,
            dma,
            dma,
            dma,
            dma((RADIUS,)),
            dma,
            dma((layers,)),
            dma,
            dma((layers,)),
            dma,
            pltpu.SemaphoreType.REGULAR,
            pltpu.SemaphoreType.REGULAR,
        ],
        compiler_params=pltpu.CompilerParams(
            collective_id=0, has_side_effects=True, vmem_limit_bytes=44 * 1024 * 1024
        ),
    )(density, pltpu.with_memory_space_constraint(mask, pltpu.HBM))
    return pl.pallas_call(
        functools.partial(closing, sizes),
        out_shape=(shape((layers, rows, width), f32),) * 2,
        in_specs=[pl.BlockSpec(memory_space=pltpu.VMEM)] * len(carried),
        out_specs=(pl.BlockSpec(memory_space=pl.ANY),) * 2,
        scratch_shapes=[
            xs,
            pltpu.VMEM((rows, width), f32),
            pltpu.VMEM((rows, width), f32),
            dma((2,)),
        ],
        compiler_params=pltpu.CompilerParams(vmem_limit_bytes=16 * 1024 * 1024),
    )(*held)


def solution(mesh):
    sizes = (mesh.shape["gz"], mesh.shape["gx"], mesh.shape["gy"])
    placed = (P("gz", "gy", "gx"), P("gz", "gy", "gx"))
    return jax.shard_map(
        functools.partial(body, sizes),
        mesh=mesh,
        in_specs=placed,
        out_specs=(P(("gz", "gx"), "gy", None), P(("gz", "gx"), "gy", None)),
        check_vma=False,
    )
```

```python
import functools
import math

import jax
import jax.numpy as jnp
from jax import lax
from jax.experimental import pallas as pl
from jax.experimental.pallas import tpu as pltpu
from jax.sharding import PartitionSpec as P

RADIUS = 6
CELLS = 8
LANES = 128
SUBLANES = 8

sharpness = 8.0
threshold = 0.5
MESH = pl.DeviceIdType.MESH


def hat(rows, cols, offset):
    row = lax.broadcasted_iota(jnp.int32, (rows, cols), 0)
    col = lax.broadcasted_iota(jnp.int32, (rows, cols), 1)
    return jnp.maximum(RADIUS + 1 - jnp.abs(col + offset - row), 0).astype(jnp.float32)


def halves(values):
    high = values.astype(jnp.bfloat16)
    low = (values - high.astype(jnp.float32)).astype(jnp.bfloat16)
    return high, low


def projection(filtered):
    top = math.tanh(sharpness * threshold)
    bottom = top + math.tanh(sharpness * (1.0 - threshold))
    return (top + jnp.tanh(sharpness * (filtered - threshold))) * (1.0 / bottom)


def one_side(reach):
    return reach * (RADIUS + 1) - reach * (reach + 1) // 2


def dot(a, b):
    return jnp.dot(a, b, preferred_element_type=jnp.float32)


def x_filter(chunks, w_own, w_edge, xs, first):
    size, columns = chunks[0].shape
    high, low = zip(*[halves(chunk) for chunk in chunks])
    none = jnp.zeros((size, LANES), jnp.bfloat16)
    for c in range(len(chunks)):
        total = dot(high[c], w_own[...]) + dot(low[c], w_own[...])
        for part in (high, low):
            left = part[c - 1][:, columns - LANES :] if c > 0 else none
            right = part[c + 1][:, :LANES] if c < len(chunks) - 1 else none
            total = total + dot(jnp.concatenate([left, right], 1), w_edge[...])
        at = pl.ds(c * columns, columns)
        xs[pl.ds(first, size), at], xs[pl.ds(first + size, size), at] = halves(total)


def y_filter(xs, scale, scale_z, columns, put):
    rows, width = scale.shape
    own = hat(rows, rows, 0).astype(jnp.bfloat16)
    edge = jnp.concatenate([hat(rows, SUBLANES, -SUBLANES), hat(rows, SUBLANES, rows)], 1)
    edge = edge.astype(jnp.bfloat16)
    own = jnp.concatenate([own, own], 1)
    edge = jnp.concatenate([edge, edge], 1)
    for c in range(width // columns):
        at = pl.ds(c * columns, columns)
        summed = dot(own, xs[pl.ds(0, 2 * rows), at])
        summed = summed + dot(edge, xs[pl.ds(2 * rows, 4 * SUBLANES), at])
        put(at, summed * (scale[:, at] * scale_z))


def inverse_count(position, length):
    left = one_side(jnp.minimum(position, RADIUS))
    right = one_side(jnp.minimum(length - 1 - position, RADIUS))
    return 1.0 / (RADIUS + 1 + left + right).astype(jnp.float32)


def layer_of(k, layers):
    return jnp.where(lax.axis_index("gx") == 0, layers - 1 - k, k)


def scale_along_z(sizes, k, layers, columns):
    nz, nx, ny = sizes
    level = (lax.axis_index("gz") * nx + lax.axis_index("gx")) * layers + layer_of(k, layers)
    level = jnp.full((SUBLANES, columns), level, jnp.int32)
    return inverse_count(level, nz * nx * layers)[0:1]


def same(ref):
    return functools.partial(pltpu.make_async_copy, ref, ref)


def wait_sides(first, second, sem, one, both):
    @pl.when(jnp.logical_and(first, second))
    def _():
        same(both)(sem).wait()

    @pl.when(first != second)
    def _():
        same(one)(sem).wait()


def kernel(
    sizes,
    density,
    mask,
    fstage,
    pstage,
    lrecv,
    lyb,
    scale,
    w_own,
    w_edge,
    phys,
    codes,
    masks,
    zf,
    recv,
    yb,
    xs,
    load_sem,
    part_sem,
    mask_sem,
    hmask_send,
    hmask_recv,
    halo_send,
    halo_recv,
    send_sem,
    recv_sem,
    y_send,
    y_recv,
    e_recv,
    relay,
    ready_y,
    ready_z,
):
    nz, nx, ny = sizes
    planes, rows, columns = density.shape
    blocks, mrows, mcols = mask.shape
    layers = planes // nx
    final = layers - 1
    gz, gx, gy = lax.axis_index("gz"), lax.axis_index("gx"), lax.axis_index("gy")
    has_up, has_down = gz > 0, gz < nz - 1
    has_prev, has_next = gy > 0, gy < ny - 1
    odd = lax.rem(gy, 2) == 1
    sides = has_prev.astype(jnp.int32) + has_next.astype(jnp.int32)

    barrier = pltpu.get_barrier_semaphore()

    def greet(sem, **where):
        pl.semaphore_signal(sem, inc=1, device_id=where, device_id_type=MESH)

    later = tuple(lax.rem(gx + p, nx) for p in (2, 3, 1))
    ahead = 2
    parts = 4
    part_rows = rows // parts

    def rows_of(q):
        return pl.ds(pl.multiple_of(q * part_rows, part_rows), part_rows)

    def load_part(q):
        return pltpu.make_async_copy(
            density.at[pl.ds(0, ahead * CELLS), rows_of(q)],
            phys.at[pl.ds(RADIUS, ahead * CELLS), rows_of(q)],
            part_sem.at[q],
        )

    def load(b):
        part = pl.ds(b * CELLS, CELLS)
        return pltpu.make_async_copy(
            density.at[part], phys.at[pl.ds(RADIUS + b * CELLS, CELLS)], load_sem.at[b - ahead]
        )

    right, left = lax.rem(gx + 1, nx), lax.rem(gx + nx - 1, nx)
    greet(barrier, gx=right)
    greet(barrier, gx=left)
    mask_copy = pltpu.make_async_copy(mask, masks.at[pl.ds(1, blocks)], mask_sem)
    mask_copy.start()
    load_part(0).start()
    pl.when(has_down)(lambda: greet(barrier, gz=gz + 1))
    pl.when(odd & has_next)(lambda: greet(barrier, gy=gy + 1))
    pl.when(odd)(lambda: greet(barrier, gy=gy - 1))
    for q in range(1, parts):
        load_part(q).start()
    for b in range(ahead, blocks):
        load(b).start()

    def to_next(j):
        return pltpu.make_async_remote_copy(
            src_ref=density.at[planes - 1 - j],
            dst_ref=phys.at[RADIUS - 1 - j],
            send_sem=halo_send,
            recv_sem=halo_recv.at[j],
            device_id={"gz": gz + 1},
            device_id_type=MESH,
        )

    def to_previous(j):
        return pltpu.make_async_remote_copy(
            src_ref=density.at[j],
            dst_ref=phys.at[RADIUS + planes + j],
            send_sem=halo_send,
            recv_sem=halo_recv.at[j],
            device_id={"gz": gz - 1},
            device_id_type=MESH,
        )

    def mask_next():
        return pltpu.make_async_remote_copy(
            src_ref=mask.at[blocks - 1],
            dst_ref=masks.at[0],
            send_sem=hmask_send,
            recv_sem=hmask_recv,
            device_id={"gz": gz + 1},
            device_id_type=MESH,
        )

    def mask_previous():
        return pltpu.make_async_remote_copy(
            src_ref=mask.at[0],
            dst_ref=masks.at[blocks + 1],
            send_sem=hmask_send,
            recv_sem=hmask_recv,
            device_id={"gz": gz - 1},
            device_id_type=MESH,
        )

    def spread(b, count):
        small = masks[pl.ds(b, count)].reshape(count * mrows, mcols)
        small = small.astype(jnp.float32).astype(jnp.bfloat16)
        c = lax.broadcasted_iota(jnp.int32, (mcols, columns), 1) // CELLS
        n = lax.broadcasted_iota(jnp.int32, (mcols, columns), 0)
        wide = jnp.where(c == n, 1.0, 0.0).astype(jnp.bfloat16)
        codes[pl.ds(b * mrows, count * mrows)] = dot(small, wide)

    def apply_rows(row, count, b, r):
        at = pl.ds(pl.multiple_of(r * CELLS, CELLS), CELLS)
        code = jnp.broadcast_to(codes[pl.ds(b * mrows + r, 1)], (CELLS, columns))
        void, solid = code < 0.5, code < 1.5
        for i in range(count):
            held = phys[row + i, at]
            phys[row + i, at] = jnp.where(void, 0.0, jnp.where(solid, 1.0, held))

    def apply_mask(row, count, b):
        def one(r, carry):
            apply_rows(row, count, b, r)
            return carry

        lax.fori_loop(0, mrows, one, 0, unroll=4 if count > 1 else 8)

    def first_piece(p, row, at):
        return pltpu.make_async_remote_copy(
            src_ref=zf.at[row, at],
            dst_ref=recv.at[0, gx, at],
            send_sem=send_sem,
            recv_sem=recv_sem.at[0],
            device_id={"gx": p},
            device_id_type=MESH,
        )

    def piece(k, p, row):
        return pltpu.make_async_remote_copy(
            src_ref=zf.at[row],
            dst_ref=recv.at[k, gx],
            send_sem=send_sem,
            recv_sem=recv_sem.at[k],
            device_id={"gx": p},
            device_id_type=MESH,
        )

    edges = (pl.ds(0, SUBLANES), pl.ds(rows - SUBLANES, SUBLANES))
    inside = pl.ds(SUBLANES, rows - 2 * SUBLANES)

    def part_piece(k, p, landing, part, sem):
        return pltpu.make_async_remote_copy(
            src_ref=zf.at[row_of(k, p), part],
            dst_ref=landing.at[gx, part],
            send_sem=send_sem,
            recv_sem=sem,
            device_id={"gx": p},
            device_id_type=MESH,
        )

    def row_of(k, p):
        if isinstance(p, int):
            return final - k if p == 0 else p * layers + k
        return jnp.where(p == 0, final - k, p * layers + k)

    def z_part(row, at, out):
        run = phys[row + RADIUS, at]
        total = run
        for d in range(1, RADIUS + 1):
            run = run + (phys[row + RADIUS - d, at] + phys[row + RADIUS + d, at])
            total = total + run
        out[at] = total

    def z_filter(row, out):
        for q in range(parts):
            z_part(row, pl.ds(q * part_rows, part_rows), out)

    def z_send(k, p):
        row = row_of(k, p)
        z_filter(row, zf.at[row])
        piece(k, p, row).start()

    def z_step(k, carry):
        for p in later:
            z_send(k, p)
        z_filter(row_of(k, gx), recv.at[k, gx])
        return carry

    parity = lax.rem(gx, 2)
    near, second, far = 1 - parity, 3 - parity, lax.rem(gx + 2, nx)

    def first_part(q, carry):
        at = rows_of(q)
        load_part(q).wait()
        for b in range(ahead):
            for r in range(mrows // parts):
                apply_rows(RADIUS + b * CELLS, CELLS, b + 1, q * (mrows // parts) + r)
        row = row_of(0, near)
        z_part(row, at, zf.at[row])
        first_piece(near, row, at).start()

        return carry

    mask_copy.wait()
    spread(1, blocks)
    pl.semaphore_wait(barrier, 2 + has_up.astype(jnp.int32) + jnp.where(odd, 0, sides))
    greet(relay, gx=left)
    lax.fori_loop(0, parts, first_part, 0)
    for b in range(ahead, blocks):
        load(b).wait()
        apply_mask(RADIUS + b * CELLS, CELLS, b + 1)
    z_send(0, second)
    pl.semaphore_wait(relay, 1)
    z_send(0, far)
    z_filter(row_of(0, gx), recv.at[0, gx])
    pl.when(has_up)(lambda: greet(ready_z, gz=gz - 1))
    pl.when(jnp.logical_not(odd) & has_prev)(lambda: greet(ready_y, gy=gy - 1))
    pl.when(jnp.logical_not(odd))(lambda: greet(ready_y, gy=gy + 1))

    @pl.when(has_up)
    def _():
        mask_previous().start()
        for j in range(RADIUS):
            to_previous(j).start()

    free = layers - RADIUS
    lax.fori_loop(1, free, z_step, 0)

    @pl.when(has_down)
    def _():
        pl.semaphore_wait(ready_z, 1)
        mask_next().start()
        for j in range(RADIUS):
            to_next(j).start()

    pl.when(odd)(lambda: pl.semaphore_wait(ready_y, sides))

    @pl.when(jnp.logical_not(has_up))
    def _():
        phys[pl.ds(0, RADIUS)] = jnp.zeros((RADIUS, rows, columns), jnp.float32)

    @pl.when(jnp.logical_not(has_down))
    def _():
        phys[pl.ds(RADIUS + planes, RADIUS)] = jnp.zeros((RADIUS, rows, columns), jnp.float32)

    @pl.when(jnp.logical_not(has_prev))
    def _():
        lyb[:, pl.ds(0, SUBLANES)] = jnp.zeros((nx, SUBLANES, columns), jnp.float32)
        yb[:, :, pl.ds(0, SUBLANES)] = jnp.zeros((final, nx, SUBLANES, columns), jnp.float32)

    @pl.when(jnp.logical_not(has_next))
    def _():
        lyb[:, pl.ds(SUBLANES, SUBLANES)] = jnp.zeros((nx, SUBLANES, columns), jnp.float32)
        yb[:, :, pl.ds(SUBLANES, SUBLANES)] = jnp.zeros((final, nx, SUBLANES, columns), jnp.float32)

    w_own[...] = hat(columns, columns, 0).astype(jnp.bfloat16)
    w_edge[pl.ds(0, LANES)] = hat(LANES, columns, LANES).astype(jnp.bfloat16)
    w_edge[pl.ds(LANES, LANES)] = hat(LANES, columns, -columns).astype(jnp.bfloat16)

    width = nx * columns
    scale_y = inverse_count(
        gy * rows + lax.broadcasted_iota(jnp.int32, (rows, LANES), 0), rows * ny
    )
    for c in range(0, width, LANES):
        lane = c + lax.broadcasted_iota(jnp.int32, (SUBLANES, LANES), 1)
        scale_x = inverse_count(lane, width)
        scale[:, pl.ds(c, LANES)] = scale_y * scale_x[0:1]

    two = pl.ds(0, 2)
    wait_sides(has_up, has_down, hmask_send, masks.at[0], masks.at[two])
    wait_sides(has_up, has_down, hmask_recv, masks.at[0], masks.at[two])
    pl.when(has_up)(lambda: spread(0, 1))
    pl.when(has_down)(lambda: spread(blocks + 1, 1))

    def take_halo(k):
        j = k - free
        wait_sides(has_up, has_down, halo_recv.at[j], zf.at[0], zf.at[two])
        pl.when(has_up)(lambda: apply_mask(RADIUS - 1 - j, 1, 0))
        pl.when(has_down)(lambda: apply_mask(RADIUS + planes + j, 1, blocks + 1))

    def halo_step(k, carry):
        take_halo(k)
        return z_step(k, carry)

    before = final - 1
    lax.fori_loop(free, before, halo_step, 0)

    last = ((before, recv.at[before]), (final, lrecv))
    for k, landing in last:
        take_halo(k)
        for p in later:
            z_filter(row_of(k, p), zf.at[row_of(k, p)])
        z_filter(row_of(k, gx), landing.at[gx])
    for k, landing in last:
        for p in later:
            for side in edges:
                part_piece(k, p, landing, side, e_recv).start()
    for k, landing in last:
        for p in later:
            part_piece(k, p, landing, inside, recv_sem.at[k]).start()

    top, bottom = pl.ds(0, SUBLANES), pl.ds(SUBLANES, SUBLANES)

    def edge_to(where, k, held, side, landing, into):
        return pltpu.make_async_remote_copy(
            src_ref=held.at[:, edges[side]],
            dst_ref=landing.at[:, into],
            send_sem=y_send,
            recv_sem=y_recv.at[k],
            device_id={"gy": where},
            device_id_type=MESH,
        )

    def send_edges(k, held, landing):
        pl.when(has_prev)(lambda: edge_to(gy - 1, k, held, 0, landing, bottom).start())
        pl.when(has_next)(lambda: edge_to(gy + 1, k, held, 1, landing, top).start())

    def take_edges(k):
        wait_sides(has_prev, has_next, y_recv.at[k], lyb.at[:, top], lyb)

    def arrive(k):
        same(zf.at[pl.ds(0, nx - 1)])(recv_sem.at[k]).wait()
        send_edges(k, recv.at[k], yb.at[k])

    def process(k):
        x_filter([recv[k, c] for c in range(nx)], w_own, w_edge, xs, 0)
        take_edges(k)
        x_filter([yb[k, c] for c in range(nx)], w_own, w_edge, xs, 2 * rows)

        def put(at, value):
            fstage[k, :, at] = value
            pstage[k, :, at] = projection(value)

        y_filter(xs, scale, scale_along_z(sizes, k, layers, columns), columns, put)

    def take_step(k, carry):
        arrive(k)
        process(k - 1)
        return carry

    def inner(k):
        same(lrecv.at[pl.ds(0, nx - 1), inside])(recv_sem.at[k]).wait()

    arrive(0)
    lax.fori_loop(1, before, take_step, 0)

    same(lrecv.at[pl.ds(0, nx - 1), pl.ds(0, 4 * SUBLANES)])(e_recv).wait()
    send_edges(before, recv.at[before], yb.at[before])
    send_edges(final, lrecv, lyb)
    process(before - 1)
    inner(before)
    process(before)

    half, whole = pl.ds(0, RADIUS), pl.ds(0, 2 * RADIUS)
    wait_sides(has_up, has_down, halo_send, zf.at[half], zf.at[whole])
    per_plane = columns * rows // (nx * SUBLANES * columns)
    half, whole = pl.ds(0, layers // per_plane), pl.ds(0, 2 * layers // per_plane)
    wait_sides(has_prev, has_next, y_send, zf.at[half], zf.at[whole])
    same(zf.at[pl.ds(0, (nx - 1) * layers)])(send_sem).wait()
    take_edges(final)
    inner(final)


def closing(sizes, fstage, pstage, lrecv, lyb, scale, w_own, w_edge, filt, proj, xs, flast, plast, sems):
    final = fstage.shape[0]
    nx, rows, columns = lrecv.shape
    layers = final + 1

    def finished(k, carry):
        at = layer_of(k, layers)
        pltpu.make_async_copy(fstage.at[k], filt.at[at], sems.at[0]).start()
        pltpu.make_async_copy(pstage.at[k], proj.at[at], sems.at[1]).start()
        return carry

    lax.fori_loop(0, final, finished, 0)
    x_filter([lrecv[c] for c in range(nx)], w_own, w_edge, xs, 0)
    x_filter([lyb[c] for c in range(nx)], w_own, w_edge, xs, 2 * rows)

    def put(at, value):
        flast[:, at] = value
        plast[:, at] = projection(value)

    y_filter(xs, scale, scale_along_z(sizes, final, layers, columns), columns, put)
    at = layer_of(final, layers)
    pltpu.make_async_copy(flast, filt.at[at], sems.at[0]).start()
    pltpu.make_async_copy(plast, proj.at[at], sems.at[1]).start()
    same(filt)(sems.at[0]).wait()
    same(proj)(sems.at[1]).wait()


def body(sizes, density, mask):
    planes, rows, columns = density.shape
    nz, nx, ny = sizes
    layers = planes // nx
    final = layers - 1
    blocks = mask.shape[0]
    width = nx * columns
    dma = pltpu.SemaphoreType.DMA
    f32, bf16 = jnp.float32, jnp.bfloat16
    shape = jax.ShapeDtypeStruct
    carried = (
        shape((final, rows, width), f32),
        shape((final, rows, width), f32),
        shape((nx, rows, columns), f32),
        shape((nx, 2 * SUBLANES, columns), f32),
        shape((rows, width), f32),
        shape((columns, columns), bf16),
        shape((2 * LANES, columns), bf16),
    )
    xs = pltpu.VMEM((2 * rows + 4 * SUBLANES, width), bf16)
    held = pl.pallas_call(
        functools.partial(kernel, sizes),
        out_shape=carried,
        in_specs=[pl.BlockSpec(memory_space=pltpu.HBM)] * 2,
        out_specs=(pl.BlockSpec(memory_space=pltpu.VMEM),) * len(carried),
        scratch_shapes=[
            pltpu.VMEM((planes + 2 * RADIUS, rows, columns), f32),
            pltpu.VMEM(((blocks + 2) * mask.shape[1], columns), f32),
            pltpu.VMEM((blocks + 2,) + mask.shape[1:], jnp.int32),
            pltpu.VMEM((planes, rows, columns), f32),
            pltpu.VMEM((final, nx, rows, columns), f32),
            pltpu.VMEM((final, nx, 2 * SUBLANES, columns), f32),
            xs,
            dma((blocks - 2,)),
            dma((4,)),
            dma,
            dma,
            dma,
            dma,
            dma((RADIUS,)),
            dma,
            dma((layers,)),
            dma,
            dma((layers,)),
            dma,
            pltpu.SemaphoreType.REGULAR,
            pltpu.SemaphoreType.REGULAR,
            pltpu.SemaphoreType.REGULAR,
        ],
        compiler_params=pltpu.CompilerParams(
            collective_id=0, has_side_effects=True, vmem_limit_bytes=44 * 1024 * 1024
        ),
    )(density, pltpu.with_memory_space_constraint(mask, pltpu.HBM))
    return pl.pallas_call(
        functools.partial(closing, sizes),
        out_shape=(shape((layers, rows, width), f32),) * 2,
        in_specs=[pl.BlockSpec(memory_space=pltpu.VMEM)] * len(carried),
        out_specs=(pl.BlockSpec(memory_space=pl.ANY),) * 2,
        scratch_shapes=[
            xs,
            pltpu.VMEM((rows, width), f32),
            pltpu.VMEM((rows, width), f32),
            dma((2,)),
        ],
        compiler_params=pltpu.CompilerParams(vmem_limit_bytes=16 * 1024 * 1024),
    )(*held)


def solution(mesh):
    sizes = (mesh.shape["gz"], mesh.shape["gx"], mesh.shape["gy"])
    placed = (P("gz", "gy", "gx"), P("gz", "gy", "gx"))
    return jax.shard_map(
        functools.partial(body, sizes),
        mesh=mesh,
        in_specs=placed,
        out_specs=(P(("gz", "gx"), "gy", None), P(("gz", "gx"), "gy", None)),
        check_vma=False,
    )
```

```python
import functools
import math

import jax
import jax.numpy as jnp
from jax import lax
from jax.experimental import pallas as pl
from jax.experimental.pallas import tpu as pltpu
from jax.sharding import PartitionSpec as P

RADIUS = 6
CELLS = 8
LANES = 128
SUBLANES = 8

sharpness = 8.0
threshold = 0.5
MESH = pl.DeviceIdType.MESH


def hat(rows, cols, offset):
    row = lax.broadcasted_iota(jnp.int32, (rows, cols), 0)
    col = lax.broadcasted_iota(jnp.int32, (rows, cols), 1)
    return jnp.maximum(RADIUS + 1 - jnp.abs(col + offset - row), 0).astype(jnp.float32)


def halves(values):
    high = values.astype(jnp.bfloat16)
    low = (values - high.astype(jnp.float32)).astype(jnp.bfloat16)
    return high, low


def projection(filtered):
    top = math.tanh(sharpness * threshold)
    bottom = top + math.tanh(sharpness * (1.0 - threshold))
    return (top + jnp.tanh(sharpness * (filtered - threshold))) * (1.0 / bottom)


def one_side(reach):
    return reach * (RADIUS + 1) - reach * (reach + 1) // 2


def dot(a, b):
    return jnp.dot(a, b, preferred_element_type=jnp.float32)


def x_filter(chunks, w_own, w_edge, xs, first):
    size, columns = chunks[0].shape
    high, low = zip(*[halves(chunk) for chunk in chunks])
    none = jnp.zeros((size, LANES), jnp.bfloat16)
    for c in range(len(chunks)):
        total = dot(high[c], w_own[...]) + dot(low[c], w_own[...])
        for part in (high, low):
            left = part[c - 1][:, columns - LANES :] if c > 0 else none
            right = part[c + 1][:, :LANES] if c < len(chunks) - 1 else none
            total = total + dot(jnp.concatenate([left, right], 1), w_edge[...])
        at = pl.ds(c * columns, columns)
        xs[pl.ds(first, size), at], xs[pl.ds(first + size, size), at] = halves(total)


def y_filter(xs, scale, scale_z, columns, put):
    rows, width = scale.shape
    own = hat(rows, rows, 0).astype(jnp.bfloat16)
    edge = jnp.concatenate([hat(rows, SUBLANES, -SUBLANES), hat(rows, SUBLANES, rows)], 1)
    edge = edge.astype(jnp.bfloat16)
    own = jnp.concatenate([own, own], 1)
    edge = jnp.concatenate([edge, edge], 1)
    for c in range(width // columns):
        at = pl.ds(c * columns, columns)
        summed = dot(own, xs[pl.ds(0, 2 * rows), at])
        summed = summed + dot(edge, xs[pl.ds(2 * rows, 4 * SUBLANES), at])
        put(at, summed * (scale[:, at] * scale_z))


def inverse_count(position, length):
    left = one_side(jnp.minimum(position, RADIUS))
    right = one_side(jnp.minimum(length - 1 - position, RADIUS))
    return 1.0 / (RADIUS + 1 + left + right).astype(jnp.float32)


def layer_of(k, layers):
    return jnp.where(lax.axis_index("gx") == 0, layers - 1 - k, k)


def scale_along_z(sizes, k, layers, columns):
    nz, nx, ny = sizes
    level = (lax.axis_index("gz") * nx + lax.axis_index("gx")) * layers + layer_of(k, layers)
    level = jnp.full((SUBLANES, columns), level, jnp.int32)
    return inverse_count(level, nz * nx * layers)[0:1]


def same(ref):
    return functools.partial(pltpu.make_async_copy, ref, ref)


def wait_sides(first, second, sem, one, both):
    @pl.when(jnp.logical_and(first, second))
    def _():
        same(both)(sem).wait()

    @pl.when(first != second)
    def _():
        same(one)(sem).wait()


def kernel(
    sizes,
    density,
    mask,
    fstage,
    pstage,
    lrecv,
    lyb,
    scale,
    w_own,
    w_edge,
    phys,
    codes,
    masks,
    zf,
    recv,
    yb,
    xs,
    load_sem,
    part_sem,
    mask_sem,
    hmask_send,
    hmask_recv,
    halo_send,
    halo_recv,
    send_sem,
    recv_sem,
    y_send,
    y_recv,
    e_recv,
    relay,
    ready_y,
    ready_z,
):
    nz, nx, ny = sizes
    planes, rows, columns = density.shape
    blocks, mrows, mcols = mask.shape
    layers = planes // nx
    final = layers - 1
    gz, gx, gy = lax.axis_index("gz"), lax.axis_index("gx"), lax.axis_index("gy")
    has_up, has_down = gz > 0, gz < nz - 1
    has_prev, has_next = gy > 0, gy < ny - 1
    odd = lax.rem(gy, 2) == 1
    sides = has_prev.astype(jnp.int32) + has_next.astype(jnp.int32)

    barrier = pltpu.get_barrier_semaphore()

    def greet(sem, **where):
        pl.semaphore_signal(sem, inc=1, device_id=where, device_id_type=MESH)

    later = tuple(lax.rem(gx + p, nx) for p in (2, 3, 1))
    ahead = 2
    parts = 4
    part_rows = rows // parts

    def rows_of(q):
        return pl.ds(pl.multiple_of(q * part_rows, part_rows), part_rows)

    def load_part(q):
        return pltpu.make_async_copy(
            density.at[pl.ds(0, ahead * CELLS), rows_of(q)],
            phys.at[pl.ds(RADIUS, ahead * CELLS), rows_of(q)],
            part_sem.at[q],
        )

    def load(b):
        part = pl.ds(b * CELLS, CELLS)
        return pltpu.make_async_copy(
            density.at[part], phys.at[pl.ds(RADIUS + b * CELLS, CELLS)], load_sem.at[b - ahead]
        )

    right, left = lax.rem(gx + 1, nx), lax.rem(gx + nx - 1, nx)
    greet(barrier, gx=right)
    greet(barrier, gx=left)
    mask_copy = pltpu.make_async_copy(mask, masks.at[pl.ds(1, blocks)], mask_sem)
    mask_copy.start()
    load_part(0).start()
    pl.when(has_down)(lambda: greet(barrier, gz=gz + 1))
    pl.when(odd & has_next)(lambda: greet(barrier, gy=gy + 1))
    pl.when(odd)(lambda: greet(barrier, gy=gy - 1))
    for q in range(1, parts):
        load_part(q).start()
    for b in range(ahead, blocks):
        load(b).start()

    def to_next(j):
        return pltpu.make_async_remote_copy(
            src_ref=density.at[planes - 1 - j],
            dst_ref=phys.at[RADIUS - 1 - j],
            send_sem=halo_send,
            recv_sem=halo_recv.at[j],
            device_id={"gz": gz + 1},
            device_id_type=MESH,
        )

    def to_previous(j):
        return pltpu.make_async_remote_copy(
            src_ref=density.at[j],
            dst_ref=phys.at[RADIUS + planes + j],
            send_sem=halo_send,
            recv_sem=halo_recv.at[j],
            device_id={"gz": gz - 1},
            device_id_type=MESH,
        )

    def mask_next():
        return pltpu.make_async_remote_copy(
            src_ref=mask.at[blocks - 1],
            dst_ref=masks.at[0],
            send_sem=hmask_send,
            recv_sem=hmask_recv,
            device_id={"gz": gz + 1},
            device_id_type=MESH,
        )

    def mask_previous():
        return pltpu.make_async_remote_copy(
            src_ref=mask.at[0],
            dst_ref=masks.at[blocks + 1],
            send_sem=hmask_send,
            recv_sem=hmask_recv,
            device_id={"gz": gz - 1},
            device_id_type=MESH,
        )

    def spread(b, count):
        small = masks[pl.ds(b, count)].reshape(count * mrows, mcols)
        small = small.astype(jnp.float32).astype(jnp.bfloat16)
        c = lax.broadcasted_iota(jnp.int32, (mcols, columns), 1) // CELLS
        n = lax.broadcasted_iota(jnp.int32, (mcols, columns), 0)
        wide = jnp.where(c == n, 1.0, 0.0).astype(jnp.bfloat16)
        codes[pl.ds(b * mrows, count * mrows)] = dot(small, wide)

    def apply_rows(row, count, b, r):
        at = pl.ds(pl.multiple_of(r * CELLS, CELLS), CELLS)
        code = jnp.broadcast_to(codes[pl.ds(b * mrows + r, 1)], (CELLS, columns))
        void, solid = code < 0.5, code < 1.5
        for i in range(count):
            held = phys[row + i, at]
            phys[row + i, at] = jnp.where(void, 0.0, jnp.where(solid, 1.0, held))

    def apply_mask(row, count, b):
        def one(r, carry):
            apply_rows(row, count, b, r)
            return carry

        lax.fori_loop(0, mrows, one, 0, unroll=4 if count > 1 else 8)

    def first_piece(p, row, at):
        return pltpu.make_async_remote_copy(
            src_ref=zf.at[row, at],
            dst_ref=recv.at[0, gx, at],
            send_sem=send_sem,
            recv_sem=recv_sem.at[0],
            device_id={"gx": p},
            device_id_type=MESH,
        )

    def piece(k, p, row):
        return pltpu.make_async_remote_copy(
            src_ref=zf.at[row],
            dst_ref=recv.at[k, gx],
            send_sem=send_sem,
            recv_sem=recv_sem.at[k],
            device_id={"gx": p},
            device_id_type=MESH,
        )

    edges = (pl.ds(0, SUBLANES), pl.ds(rows - SUBLANES, SUBLANES))
    inside = pl.ds(SUBLANES, rows - 2 * SUBLANES)

    def part_piece(k, p, landing, part, sem):
        return pltpu.make_async_remote_copy(
            src_ref=zf.at[row_of(k, p), part],
            dst_ref=landing.at[gx, part],
            send_sem=send_sem,
            recv_sem=sem,
            device_id={"gx": p},
            device_id_type=MESH,
        )

    def row_of(k, p):
        if isinstance(p, int):
            return final - k if p == 0 else p * layers + k
        return jnp.where(p == 0, final - k, p * layers + k)

    def z_part(row, at, out):
        run = phys[row + RADIUS, at]
        total = run
        for d in range(1, RADIUS + 1):
            run = run + (phys[row + RADIUS - d, at] + phys[row + RADIUS + d, at])
            total = total + run
        out[at] = total

    def z_filter(row, out):
        for q in range(parts):
            z_part(row, pl.ds(q * part_rows, part_rows), out)

    def z_send(k, p):
        row = row_of(k, p)
        z_filter(row, zf.at[row])
        piece(k, p, row).start()

    def z_step(k, carry):
        for p in later:
            z_send(k, p)
        z_filter(row_of(k, gx), recv.at[k, gx])
        return carry

    parity = lax.rem(gx, 2)
    near, second, far = 1 - parity, 3 - parity, lax.rem(gx + 2, nx)

    def first_part(q, carry):
        at = rows_of(q)
        load_part(q).wait()
        for b in range(ahead):
            for r in range(mrows // parts):
                apply_rows(RADIUS + b * CELLS, CELLS, b + 1, q * (mrows // parts) + r)
        row = row_of(0, near)
        z_part(row, at, zf.at[row])
        first_piece(near, row, at).start()

        return carry

    mask_copy.wait()
    spread(1, blocks)
    pl.semaphore_wait(barrier, 2 + has_up.astype(jnp.int32) + jnp.where(odd, 0, sides))
    greet(relay, gx=left)
    lax.fori_loop(0, parts, first_part, 0)
    for b in range(ahead, blocks):
        load(b).wait()
        apply_mask(RADIUS + b * CELLS, CELLS, b + 1)
        pl.when(second == b)(lambda: z_send(0, second))
    pl.semaphore_wait(relay, 1)
    z_send(0, far)
    z_filter(row_of(0, gx), recv.at[0, gx])
    pl.when(has_up)(lambda: greet(ready_z, gz=gz - 1))
    pl.when(jnp.logical_not(odd) & has_prev)(lambda: greet(ready_y, gy=gy - 1))
    pl.when(jnp.logical_not(odd))(lambda: greet(ready_y, gy=gy + 1))

    @pl.when(has_up)
    def _():
        mask_previous().start()
        for j in range(RADIUS):
            to_previous(j).start()

    free = layers - RADIUS
    lax.fori_loop(1, free, z_step, 0)

    @pl.when(has_down)
    def _():
        pl.semaphore_wait(ready_z, 1)
        mask_next().start()
        for j in range(RADIUS):
            to_next(j).start()

    pl.when(odd)(lambda: pl.semaphore_wait(ready_y, sides))

    @pl.when(jnp.logical_not(has_up))
    def _():
        phys[pl.ds(0, RADIUS)] = jnp.zeros((RADIUS, rows, columns), jnp.float32)

    @pl.when(jnp.logical_not(has_down))
    def _():
        phys[pl.ds(RADIUS + planes, RADIUS)] = jnp.zeros((RADIUS, rows, columns), jnp.float32)

    @pl.when(jnp.logical_not(has_prev))
    def _():
        lyb[:, pl.ds(0, SUBLANES)] = jnp.zeros((nx, SUBLANES, columns), jnp.float32)
        yb[:, :, pl.ds(0, SUBLANES)] = jnp.zeros((final, nx, SUBLANES, columns), jnp.float32)

    @pl.when(jnp.logical_not(has_next))
    def _():
        lyb[:, pl.ds(SUBLANES, SUBLANES)] = jnp.zeros((nx, SUBLANES, columns), jnp.float32)
        yb[:, :, pl.ds(SUBLANES, SUBLANES)] = jnp.zeros((final, nx, SUBLANES, columns), jnp.float32)

    w_own[...] = hat(columns, columns, 0).astype(jnp.bfloat16)
    w_edge[pl.ds(0, LANES)] = hat(LANES, columns, LANES).astype(jnp.bfloat16)
    w_edge[pl.ds(LANES, LANES)] = hat(LANES, columns, -columns).astype(jnp.bfloat16)

    width = nx * columns
    scale_y = inverse_count(
        gy * rows + lax.broadcasted_iota(jnp.int32, (rows, LANES), 0), rows * ny
    )
    for c in range(0, width, LANES):
        lane = c + lax.broadcasted_iota(jnp.int32, (SUBLANES, LANES), 1)
        scale_x = inverse_count(lane, width)
        scale[:, pl.ds(c, LANES)] = scale_y * scale_x[0:1]

    two = pl.ds(0, 2)
    wait_sides(has_up, has_down, hmask_send, masks.at[0], masks.at[two])
    wait_sides(has_up, has_down, hmask_recv, masks.at[0], masks.at[two])
    pl.when(has_up)(lambda: spread(0, 1))
    pl.when(has_down)(lambda: spread(blocks + 1, 1))

    def take_halo(k):
        j = k - free
        wait_sides(has_up, has_down, halo_recv.at[j], zf.at[0], zf.at[two])
        pl.when(has_up)(lambda: apply_mask(RADIUS - 1 - j, 1, 0))
        pl.when(has_down)(lambda: apply_mask(RADIUS + planes + j, 1, blocks + 1))

    def halo_step(k, carry):
        take_halo(k)
        return z_step(k, carry)

    before = final - 1
    lax.fori_loop(free, before, halo_step, 0)

    last = ((before, recv.at[before]), (final, lrecv))
    for k, landing in last:
        take_halo(k)
        for p in later:
            z_filter(row_of(k, p), zf.at[row_of(k, p)])
        z_filter(row_of(k, gx), landing.at[gx])
    for k, landing in last:
        for p in later:
            for side in edges:
                part_piece(k, p, landing, side, e_recv).start()
    for k, landing in last:
        for p in later:
            part_piece(k, p, landing, inside, recv_sem.at[k]).start()

    top, bottom = pl.ds(0, SUBLANES), pl.ds(SUBLANES, SUBLANES)

    def edge_to(where, k, held, side, landing, into):
        return pltpu.make_async_remote_copy(
            src_ref=held.at[:, edges[side]],
            dst_ref=landing.at[:, into],
            send_sem=y_send,
            recv_sem=y_recv.at[k],
            device_id={"gy": where},
            device_id_type=MESH,
        )

    def send_edges(k, held, landing):
        pl.when(has_prev)(lambda: edge_to(gy - 1, k, held, 0, landing, bottom).start())
        pl.when(has_next)(lambda: edge_to(gy + 1, k, held, 1, landing, top).start())

    def take_edges(k):
        wait_sides(has_prev, has_next, y_recv.at[k], lyb.at[:, top], lyb)

    def arrive(k):
        same(zf.at[pl.ds(0, nx - 1)])(recv_sem.at[k]).wait()
        send_edges(k, recv.at[k], yb.at[k])

    def process(k):
        x_filter([recv[k, c] for c in range(nx)], w_own, w_edge, xs, 0)
        take_edges(k)
        x_filter([yb[k, c] for c in range(nx)], w_own, w_edge, xs, 2 * rows)

        def put(at, value):
            fstage[k, :, at] = value
            pstage[k, :, at] = projection(value)

        y_filter(xs, scale, scale_along_z(sizes, k, layers, columns), columns, put)

    def take_step(k, carry):
        arrive(k)
        process(k - 1)
        return carry

    def inner(k):
        same(lrecv.at[pl.ds(0, nx - 1), inside])(recv_sem.at[k]).wait()

    arrive(0)
    lax.fori_loop(1, before, take_step, 0)

    same(lrecv.at[pl.ds(0, nx - 1), pl.ds(0, 4 * SUBLANES)])(e_recv).wait()
    send_edges(before, recv.at[before], yb.at[before])
    send_edges(final, lrecv, lyb)
    process(before - 1)
    inner(before)
    process(before)

    half, whole = pl.ds(0, RADIUS), pl.ds(0, 2 * RADIUS)
    wait_sides(has_up, has_down, halo_send, zf.at[half], zf.at[whole])
    per_plane = columns * rows // (nx * SUBLANES * columns)
    half, whole = pl.ds(0, layers // per_plane), pl.ds(0, 2 * layers // per_plane)
    wait_sides(has_prev, has_next, y_send, zf.at[half], zf.at[whole])
    same(zf.at[pl.ds(0, (nx - 1) * layers)])(send_sem).wait()
    take_edges(final)
    inner(final)


def closing(sizes, fstage, pstage, lrecv, lyb, scale, w_own, w_edge, filt, proj, xs, flast, plast, sems):
    final = fstage.shape[0]
    nx, rows, columns = lrecv.shape
    layers = final + 1

    def finished(k, carry):
        at = layer_of(k, layers)
        pltpu.make_async_copy(fstage.at[k], filt.at[at], sems.at[0]).start()
        pltpu.make_async_copy(pstage.at[k], proj.at[at], sems.at[1]).start()
        return carry

    lax.fori_loop(0, final, finished, 0)
    x_filter([lrecv[c] for c in range(nx)], w_own, w_edge, xs, 0)
    x_filter([lyb[c] for c in range(nx)], w_own, w_edge, xs, 2 * rows)

    def put(at, value):
        flast[:, at] = value
        plast[:, at] = projection(value)

    y_filter(xs, scale, scale_along_z(sizes, final, layers, columns), columns, put)
    at = layer_of(final, layers)
    pltpu.make_async_copy(flast, filt.at[at], sems.at[0]).start()
    pltpu.make_async_copy(plast, proj.at[at], sems.at[1]).start()
    same(filt)(sems.at[0]).wait()
    same(proj)(sems.at[1]).wait()


def body(sizes, density, mask):
    planes, rows, columns = density.shape
    nz, nx, ny = sizes
    layers = planes // nx
    final = layers - 1
    blocks = mask.shape[0]
    width = nx * columns
    dma = pltpu.SemaphoreType.DMA
    f32, bf16 = jnp.float32, jnp.bfloat16
    shape = jax.ShapeDtypeStruct
    carried = (
        shape((final, rows, width), f32),
        shape((final, rows, width), f32),
        shape((nx, rows, columns), f32),
        shape((nx, 2 * SUBLANES, columns), f32),
        shape((rows, width), f32),
        shape((columns, columns), bf16),
        shape((2 * LANES, columns), bf16),
    )
    xs = pltpu.VMEM((2 * rows + 4 * SUBLANES, width), bf16)
    held = pl.pallas_call(
        functools.partial(kernel, sizes),
        out_shape=carried,
        in_specs=[pl.BlockSpec(memory_space=pltpu.HBM)] * 2,
        out_specs=(pl.BlockSpec(memory_space=pltpu.VMEM),) * len(carried),
        scratch_shapes=[
            pltpu.VMEM((planes + 2 * RADIUS, rows, columns), f32),
            pltpu.VMEM(((blocks + 2) * mask.shape[1], columns), f32),
            pltpu.VMEM((blocks + 2,) + mask.shape[1:], jnp.int32),
            pltpu.VMEM((planes, rows, columns), f32),
            pltpu.VMEM((final, nx, rows, columns), f32),
            pltpu.VMEM((final, nx, 2 * SUBLANES, columns), f32),
            xs,
            dma((blocks - 2,)),
            dma((4,)),
            dma,
            dma,
            dma,
            dma,
            dma((RADIUS,)),
            dma,
            dma((layers,)),
            dma,
            dma((layers,)),
            dma,
            pltpu.SemaphoreType.REGULAR,
            pltpu.SemaphoreType.REGULAR,
            pltpu.SemaphoreType.REGULAR,
        ],
        compiler_params=pltpu.CompilerParams(
            collective_id=0, has_side_effects=True, vmem_limit_bytes=44 * 1024 * 1024
        ),
    )(density, pltpu.with_memory_space_constraint(mask, pltpu.HBM))
    return pl.pallas_call(
        functools.partial(closing, sizes),
        out_shape=(shape((layers, rows, width), f32),) * 2,
        in_specs=[pl.BlockSpec(memory_space=pltpu.VMEM)] * len(carried),
        out_specs=(pl.BlockSpec(memory_space=pl.ANY),) * 2,
        scratch_shapes=[
            xs,
            pltpu.VMEM((rows, width), f32),
            pltpu.VMEM((rows, width), f32),
            dma((2,)),
        ],
        compiler_params=pltpu.CompilerParams(vmem_limit_bytes=16 * 1024 * 1024),
    )(*held)


def solution(mesh):
    sizes = (mesh.shape["gz"], mesh.shape["gx"], mesh.shape["gy"])
    placed = (P("gz", "gy", "gx"), P("gz", "gy", "gx"))
    return jax.shard_map(
        functools.partial(body, sizes),
        mesh=mesh,
        in_specs=placed,
        out_specs=(P(("gz", "gx"), "gy", None), P(("gz", "gx"), "gy", None)),
        check_vma=False,
    )
```
